16 devices in a mesh: rep: 1, dp: 16 (over x, y, z, core).
Axes of the slice: x: 2, y: 2, z: 2, core: 2. Of those that a mesh axis runs over, the one named last changes fastest.
Arguments:
- g_w_gate: bfloat16 [16, 2, 1024, 2816], P(('rep', 'dp'))
- g_w_up: bfloat16 [16, 2, 1024, 2816], P(('rep', 'dp'))
- g_w_down: bfloat16 [16, 2, 2816, 1024], P(('rep', 'dp'))
- w_gate: bfloat16 [2, 1024, 2816], replicated
- w_up: bfloat16 [2, 1024, 2816], replicated
- w_down: bfloat16 [2, 2816, 1024], replicated
- m_w_gate: float32 [2, 1024, 2816], P(None, 'dp')
- m_w_up: float32 [2, 1024, 2816], P(None, 'dp')
- m_w_down: float32 [2, 2816, 1024], P(None, 'dp')
- v_w_gate: float32 [2, 1024, 2816], P(None, 'dp')
- v_w_up: float32 [2, 1024, 2816], P(None, 'dp')
- v_w_down: float32 [2, 2816, 1024], P(None, 'dp')
Outputs:
- output 1: bfloat16 [2, 1024, 2816], P('rep')
- output 2: bfloat16 [2, 1024, 2816], P('rep')
- output 3: bfloat16 [2, 2816, 1024], P('rep')
- output 4: float32 [2, 1024, 2816], P('rep', 'dp')
- output 5: float32 [2, 1024, 2816], P('rep', 'dp')
- output 6: float32 [2, 2816, 1024], P('rep', 'dp')
- output 7: float32 [2, 1024, 2816], P('rep', 'dp')
- output 8: float32 [2, 1024, 2816], P('rep', 'dp')
- output 9: float32 [2, 2816, 1024], P('rep', 'dp')
All inputs are finite; a program needn't handle non-finite values.
Results may differ from the reference program's by a relative error of at most 0.022.
Values are sent between devices in bfloat16 or wider.
A program may use at most 2 GiB of HBM per device.

```python
import jax
import jax.numpy as jnp
from jax import lax

DEVICES = 16
D = 1024
FF = 2816
LAYERS = 2
NAMES = ("w_gate", "w_up", "w_down")
SHAPES = {"w_gate": (LAYERS, D, FF), "w_up": (LAYERS, D, FF), "w_down": (LAYERS, FF, D)}


def setup_inputs(seed: int = 0, part: int = 0) -> dict:
    kz, *keys = jax.random.split(jax.random.key(seed), 1 + 5 * len(NAMES))
    loud = 2.0 ** jax.random.uniform(kz, (), jnp.float32, -1.0, 1.0)
    drawn = {}
    for name, key, both in zip(NAMES, keys[:3], keys[3:6], strict=True):
        own = jax.random.normal(jax.random.fold_in(key, part), (DEVICES, *SHAPES[name]), jnp.float32)
        shared = jax.random.normal(jax.random.fold_in(both, part), SHAPES[name], jnp.float32)
        drawn["g_" + name] = (loud * (0.7 * shared / DEVICES + 0.7 * own * DEVICES**-0.5)).astype(jnp.bfloat16)
    for name, key in zip(NAMES, keys[6:9], strict=True):
        drawn[name] = (jax.random.normal(key, SHAPES[name], jnp.float32) * SHAPES[name][1] ** -0.5).astype(jnp.bfloat16)
    for name, key in zip(NAMES, keys[9:12], strict=True):
        drawn["m_" + name] = loud * 0.5 * jax.random.normal(key, SHAPES[name], jnp.float32)
    for name, key in zip(NAMES, keys[12:15], strict=True):
        drawn["v_" + name] = loud * loud * jax.random.uniform(key, SHAPES[name], jnp.float32, 0.5, 1.5)
    return drawn


def adamw(w, m, v, g):
    m = 0.9 * m + 0.1 * g
    v = 0.95 * v + 0.05 * g * g
    step = m * lax.rsqrt(v + 1e-8) + 0.1 * w
    return (w - 0.02 * step).astype(jnp.bfloat16), m, v


def reference(g_w_gate, g_w_up, g_w_down, w_gate, w_up, w_down, m_w_gate, m_w_up, m_w_down, v_w_gate, v_w_up, v_w_down):
    def total(terms):
        return lax.scan(lambda so_far, term: (so_far + term.astype(jnp.float32), None), jnp.zeros(terms.shape[1:], jnp.float32), terms)[0]

    gradients = [total(terms).astype(jnp.bfloat16).astype(jnp.float32) for terms in (g_w_gate, g_w_up, g_w_down)]
    new = [
        adamw(w.astype(jnp.float32), m, v, g)
        for w, m, v, g in zip((w_gate, w_up, w_down), (m_w_gate, m_w_up, m_w_down), (v_w_gate, v_w_up, v_w_down), gradients, strict=True)
    ]
    return tuple(one[which] for which in range(3) for one in new)
```

```python
import jax
import jax.numpy as jnp
from jax import lax
from jax.experimental import pallas as pl
from jax.experimental.pallas import tpu as pltpu
from jax.sharding import PartitionSpec as P

BF16, F32 = jnp.bfloat16, jnp.float32
MESH = pl.DeviceIdType.MESH
LAYERS = 2
ORDERS = ((0, 1, 2), (1, 2, 0), (2, 0, 1))
STRIDES = (8, 4, 2)
SLAB = 16


def adamw(w, m, v, g):
    m = 0.9 * m + 0.1 * g
    v = 0.95 * v + 0.05 * g * g
    step = m * lax.rsqrt(v + 1e-8) + 0.1 * w
    return (w - 0.02 * step).astype(BF16), m, v


class Weight:
    def __init__(self, order, where, core, **refs):
        self.order, self.core = order, core
        self.mine = [where[axis] for axis in order]
        self.__dict__.update(refs)

    def place(self, *stages):
        xyz = [None] * 3
        for axis, coordinate in zip(self.order, stages, strict=True):
            xyz[axis] = coordinate
        return tuple(xyz)

    def block(self, keep1, keep2, keep3):
        return self.place(*(1 - m + k * (2 * m - 1) for m, k in zip(self.mine, (keep1, keep2, keep3), strict=True)))


def kernel(*refs):
    g_refs, w_refs, m_refs, v_refs = (refs[i : i + 3] for i in (0, 3, 6, 9))
    all_refs, m_outs, v_outs = (refs[i : i + 3] for i in (12, 15, 18))
    firsts, seconds, thirds, olds = (refs[i : i + 3] for i in (21, 24, 27, 30))
    load_sem, rest_sem, mv_sem, pair_sem, s1_sem, s2_sem, s3_sem, a3_sem, a2_sem, a1_sem, a0_sem, send_sem, third_sem, free_sem, read_sem = refs[33:]

    me = lax.axis_index("dp")
    core = me % 2
    where = [(me // s) % 2 for s in STRIDES]
    partners = [me + s * (1 - 2 * b) for s, b in zip(STRIDES, where, strict=True)]
    pair = me + 1 - 2 * core

    weights = [
        Weight(
            ORDERS[i], where, core, i=i, g=g_refs[i], all=all_refs[i], m=m_outs[i], v=v_outs[i],
            first=firsts[i], second=seconds[i], third=thirds[i], old=olds[i],
            to=[partners[axis] for axis in ORDERS[i]],
        )
        for i in range(3)
    ]

    def remote(src, dst, send, recv, device):
        return pltpu.make_async_remote_copy(
            src_ref=src, dst_ref=dst, send_sem=send, recv_sem=recv, device_id={"dp": device}, device_id_type=MESH
        )

    def unit(w, keep1, k):
        return (k % 2, *w.block(keep1, k // 4, (k // 2) % 2))

    def load(w, k):
        at = (*unit(w, 0, k), core)
        return pltpu.make_async_copy(w.g.at[at], w.all.at[at], load_sem.at[w.i, k])

    def load_rest(w):
        at = (slice(None), *w.place(w.mine[0], slice(None), slice(None)), core)
        return pltpu.make_async_copy(w.g.at[at], w.all.at[at], rest_sem.at[w.i])

    def own_block(w):
        return (slice(None), *w.block(1, 1, 1), core)

    def moments(w):
        i = w.i
        return (
            pltpu.make_async_copy(m_refs[i], w.m, mv_sem.at[i, 0]),
            pltpu.make_async_copy(v_refs[i], w.v, mv_sem.at[i, 1]),
            pltpu.make_async_copy(w_refs[i].at[own_block(w)], w.old, mv_sem.at[i, 2]),
        )

    def to_pair(w, keep1, k):
        at = unit(w, keep1, k)
        return remote(w.g.at[(*at, 1 - core)], w.all.at[(*at, core)], send_sem.at[w.i, 0], pair_sem.at[w.i, 8 * keep1 + k], pair)

    def first(w, k):
        at = unit(w, 0, k)
        return remote(w.all.at[(*at, core)], w.first.at[k], send_sem.at[w.i, 1], s1_sem.at[w.i, k], w.to[0])

    def second(w, k):
        at = (k % 2, *w.block(1, 0, k // 2))
        return remote(w.all.at[(*at, core)], w.second.at[k], send_sem.at[w.i, 2], s2_sem.at[w.i, k], w.to[1])

    def third(w, k):
        at = (k, *w.block(1, 1, 0))
        return remote(w.all.at[(*at, core)], w.third.at[k], third_sem.at[w.i, k], s3_sem.at[w.i, k], w.to[2])

    def tell(w, stage):
        pl.semaphore_signal(free_sem.at[w.i, stage], inc=1, device_id={"dp": w.to[stage]}, device_id_type=MESH)

    def told(w, stage):
        pl.semaphore_wait(free_sem.at[w.i, stage], 1)

    def gather3(w, k):
        at = (k, *w.block(1, 1, 1), core)
        return remote(w.all.at[at], w.all.at[at], send_sem.at[w.i, 4], a3_sem.at[w.i, k], w.to[2])

    def gather2(w, k):
        at = (k % 2, *w.block(1, 1, 1 - k // 2), core)
        return remote(w.all.at[at], w.all.at[at], send_sem.at[w.i, 5], a2_sem.at[w.i, k], w.to[1])

    def gather1(w, k):
        at = (k % 2, *w.block(1, 1 - k // 4, 1 - (k // 2) % 2), core)
        return remote(w.all.at[at], w.all.at[at], send_sem.at[w.i, 6], a1_sem.at[w.i, k], w.to[0])

    def gather0(w, keep1, k):
        at = (k % 2, *w.block(keep1, 1 - k // 4, 1 - (k // 2) % 2), core)
        return remote(w.all.at[at], w.all.at[at], send_sem.at[w.i, 7], a0_sem.at[w.i], pair)

    def total(w, at, rows, *others):
        sum_ = w.all[(*at, core, rows, slice(None))].astype(F32) + w.all[(*at, 1 - core, rows, slice(None))].astype(F32)
        for other, k in others:
            sum_ = sum_ + other[k, rows, :].astype(F32)
        return sum_

    def add(w, at, *others):
        @pl.loop(0, w.old.shape[1] // SLAB)
        def _(r):
            rows = pl.ds(pl.multiple_of(r * SLAB, SLAB), SLAB)
            w.all[(*at, core, rows, slice(None))] = total(w, at, rows, *others).astype(BF16)

    def each(n, body):
        @pl.loop(0, n)
        def _(k):
            body(k)

    def start_loads(k):
        for w in weights:
            load(w, k).start()

    each(8, start_loads)

    barrier = pltpu.get_barrier_semaphore()
    for device in (pair, *partners):
        pl.semaphore_signal(barrier, inc=1, device_id={"dp": device}, device_id_type=MESH)
    pl.semaphore_wait(barrier, 4)

    for keep1 in (0, 1):

        def start_pair(k, keep1=keep1):
            for w in weights:
                to_pair(w, keep1, k).start()

        each(8, start_pair)
    for w in weights:
        load_rest(w).start()
    for w in weights:
        for copy in moments(w):
            copy.start()

    def stage1(k):
        for w in weights:
            load(w, k).wait()
            to_pair(w, 0, k).wait_recv()
            add(w, unit(w, 0, k))
        for w in weights:
            first(w, k).start()

    each(8, stage1)
    for w in weights:
        load_rest(w).wait()

    def stage2(k):
        for w in weights:
            to_pair(w, 1, k).wait_recv()
            first(w, k).wait_recv()
            add(w, unit(w, 1, k), (w.first, k))
        for w in weights:
            second(w, k).start()

    each(4, stage2)

    def stage3(k):
        for w in weights:
            to_pair(w, 1, 4 + k).wait_recv()
            first(w, 4 + k).wait_recv()
            second(w, k).wait_recv()
            add(w, unit(w, 1, 4 + k), (w.first, 4 + k), (w.second, k))
        for w in weights:
            third(w, k).start()

    each(2, stage3)
    for w in weights:
        for copy in moments(w):
            copy.wait()
        remote(w.first, w.first, send_sem.at[w.i, 1], s1_sem.at[w.i, 0], pair).wait_send()
        tell(w, 0)
        remote(w.second, w.second, send_sem.at[w.i, 2], s2_sem.at[w.i, 0], pair).wait_send()
        tell(w, 1)

    def update(k):
        for w in weights:
            to_pair(w, 1, 6 + k).wait_recv()
            first(w, 6 + k).wait_recv()
            second(w, 2 + k).wait_recv()
            third(w, k).wait()
            tell(w, 2)
            at = (k, *w.block(1, 1, 1))

            @pl.loop(0, w.old.shape[1] // SLAB)
            def _(r, w=w, at=at):
                rows = pl.ds(pl.multiple_of(r * SLAB, SLAB), SLAB)
                g = total(w, at, rows, (w.first, 6 + k), (w.second, 2 + k), (w.third, k)).astype(BF16).astype(F32)
                new, m, v = adamw(w.old[k, rows, :].astype(F32), w.m[k, rows, :], w.v[k, rows, :], g)
                w.m[k, rows, :] = m
                w.v[k, rows, :] = v
                w.all[(*at, core, rows, slice(None))] = new

        for w in weights:
            told(w, 2)
            gather3(w, k).start()

    each(2, update)

    def own21(k):
        for w in weights:
            gather2(w, k).start()
        for w in weights:
            gather1(w, k).start()

    for w in weights:
        told(w, 1)
        told(w, 0)
    each(2, own21)

    pl.semaphore_signal(read_sem, inc=1, device_id={"dp": pair}, device_id_type=MESH)
    pl.semaphore_wait(read_sem, 1)

    def own(k):
        for w in weights:
            gather0(w, 1, k).start()

    each(2, own)

    def back3(k):
        for w in weights:
            gather3(w, k).wait_recv()
            gather2(w, 2 + k).start()
        for w in weights:
            gather1(w, 2 + k).start()
            gather0(w, 1, 2 + k).start()

    each(2, back3)

    def back2(k):
        for w in weights:
            gather2(w, k).wait_recv()
            gather1(w, 4 + k).start()
            gather0(w, 1, 4 + k).start()

    each(4, back2)

    def back1(k):
        for w in weights:
            gather1(w, k).wait_recv()
            gather0(w, 0, k).start()

    each(8, back1)

    for w in weights:
        theirs = w.all.at[:, :, :, :, 1 - core]
        remote(theirs, theirs, send_sem.at[w.i, 7], a0_sem.at[w.i], pair).wait_recv()
    for w in weights:
        mine = w.all.at[:, :, :, :, core]
        for n, ref in ((0, mine), (4, w.third), (5, w.second), (6, w.first), (7, mine)):
            remote(ref, ref, send_sem.at[w.i, n], a0_sem.at[w.i], pair).wait_send()


def put(*refs):
    sem = refs[-1]
    copies = [
        pltpu.make_async_copy(refs[i].at[k], refs[9 + i].at[k], sem.at[i, k]) for i in range(9) for k in range(LAYERS)
    ]
    for copy in copies:
        copy.start()
    for copy in copies:
        copy.wait()


def solution(mesh):
    def step(*arrays):
        shapes = [a.shape[1:] for a in arrays[6:9]]

        def cut(a, i):
            return a.reshape(LAYERS, 2, 2, 2, 2, *shapes[i])

        operands = [cut(a, n % 3) for n, a in enumerate(arrays[:6])] + list(arrays[6:])
        blocks = [(n, rows, columns) for n in (8, 4, 2, LAYERS) for rows, columns in shapes]
        outs = pl.pallas_call(
            kernel,
            out_shape=[pltpu.VMEM((LAYERS, 2, 2, 2, 2, *s), BF16) for s in shapes] + [pltpu.VMEM((LAYERS, *s), F32) for s in shapes] * 2,
            in_specs=[pl.BlockSpec(memory_space=pl.ANY)] * 12,
            out_specs=[pl.BlockSpec(memory_space=pltpu.VMEM)] * 9,
            scratch_shapes=[
                *(pltpu.VMEM(s, BF16) for s in blocks),
                pltpu.SemaphoreType.DMA((3, 8)),
                pltpu.SemaphoreType.DMA((3,)),
                pltpu.SemaphoreType.DMA((3, 3)),
                pltpu.SemaphoreType.DMA((3, 16)),
                pltpu.SemaphoreType.DMA((3, 8)),
                pltpu.SemaphoreType.DMA((3, 4)),
                pltpu.SemaphoreType.DMA((3, 2)),
                pltpu.SemaphoreType.DMA((3, 2)),
                pltpu.SemaphoreType.DMA((3, 4)),
                pltpu.SemaphoreType.DMA((3, 8)),
                pltpu.SemaphoreType.DMA((3,)),
                pltpu.SemaphoreType.DMA((3, 8)),
                pltpu.SemaphoreType.DMA((3, 2)),
                pltpu.SemaphoreType.REGULAR((3, 3)),
                pltpu.SemaphoreType.REGULAR,
            ],
            compiler_params=pltpu.CompilerParams(collective_id=0, has_side_effects=True, vmem_limit_bytes=20 * 1024 * 1024),
            name="step",
        )(*operands)
        done = pl.pallas_call(
            put,
            out_shape=[jax.ShapeDtypeStruct(o.shape, o.dtype) for o in outs],
            in_specs=[pl.BlockSpec(memory_space=pl.ANY)] * 9,
            out_specs=[pl.BlockSpec(memory_space=pl.ANY)] * 9,
            scratch_shapes=[pltpu.SemaphoreType.DMA((9, LAYERS))],
            compiler_params=pltpu.CompilerParams(vmem_limit_bytes=1024 * 1024),
            name="put",
        )(*outs)
        whole = [o.reshape(a.shape) for o, a in zip(done[:3], arrays[3:6], strict=True)]
        return (*whole, *done[3:])

    all_of, part = P(None, None, None), P(None, "dp", None)
    return jax.shard_map(
        step,
        mesh=mesh,
        in_specs=(P(("rep", "dp"), None, None, None),) * 3 + (all_of,) * 3 + (part,) * 6,
        out_specs=(P("rep", None, None),) * 3 + (P("rep", "dp", None),) * 6,
        check_vma=False,
    )
```

```python
import jax
import jax.numpy as jnp
from jax import lax
from jax.experimental import pallas as pl
from jax.experimental.pallas import tpu as pltpu
from jax.sharding import PartitionSpec as P

BF16, F32 = jnp.bfloat16, jnp.float32
MESH = pl.DeviceIdType.MESH
LAYERS = 2
ORDERS = ((0, 1, 2), (1, 2, 0), (2, 0, 1))
STRIDES = (8, 4, 2)
SLAB = 16


def adamw(w, m, v, g):
    m = 0.9 * m + 0.1 * g
    v = 0.95 * v + 0.05 * g * g
    step = m * lax.rsqrt(v + 1e-8) + 0.1 * w
    return (w - 0.02 * step).astype(BF16), m, v


class Weight:
    def __init__(self, order, where, core, **refs):
        self.order, self.core = order, core
        self.mine = [where[axis] for axis in order]
        self.__dict__.update(refs)

    def place(self, *stages):
        xyz = [None] * 3
        for axis, coordinate in zip(self.order, stages, strict=True):
            xyz[axis] = coordinate
        return tuple(xyz)

    def block(self, keep1, keep2, keep3):
        return self.place(*(1 - m + k * (2 * m - 1) for m, k in zip(self.mine, (keep1, keep2, keep3), strict=True)))


def kernel(*refs):
    g_refs, w_refs, m_refs, v_refs = (refs[i : i + 3] for i in (0, 3, 6, 9))
    all_refs, m_outs, v_outs = (refs[i : i + 3] for i in (12, 15, 18))
    firsts, seconds, thirds, olds = (refs[i : i + 3] for i in (21, 24, 27, 30))
    load_sem, rest_sem, mv_sem, pair_sem, s1_sem, s2_sem, s3_sem, a3_sem, a2_sem, a1_sem, a0_sem, send_sem, third_sem, free_sem, read_sem = refs[33:]

    me = lax.axis_index("dp")
    core = me % 2
    where = [(me // s) % 2 for s in STRIDES]
    partners = [me + s * (1 - 2 * b) for s, b in zip(STRIDES, where, strict=True)]
    pair = me + 1 - 2 * core

    weights = [
        Weight(
            ORDERS[i], where, core, i=i, g=g_refs[i], all=all_refs[i], m=m_outs[i], v=v_outs[i],
            first=firsts[i], second=seconds[i], third=thirds[i], old=olds[i],
            to=[partners[axis] for axis in ORDERS[i]],
        )
        for i in range(3)
    ]

    def remote(src, dst, send, recv, device):
        return pltpu.make_async_remote_copy(
            src_ref=src, dst_ref=dst, send_sem=send, recv_sem=recv, device_id={"dp": device}, device_id_type=MESH
        )

    def unit(w, keep1, k):
        return (k % 2, *w.block(keep1, k // 4, (k // 2) % 2))

    def load(w, k):
        at = (*unit(w, 0, k), core)
        return pltpu.make_async_copy(w.g.at[at], w.all.at[at], load_sem.at[w.i, k])

    def load_rest(w):
        at = (slice(None), *w.place(w.mine[0], slice(None), slice(None)), core)
        return pltpu.make_async_copy(w.g.at[at], w.all.at[at], rest_sem.at[w.i])

    def own_block(w):
        return (slice(None), *w.block(1, 1, 1), core)

    def moments(w):
        i = w.i
        return (
            pltpu.make_async_copy(m_refs[i], w.m, mv_sem.at[i, 0]),
            pltpu.make_async_copy(v_refs[i], w.v, mv_sem.at[i, 1]),
            pltpu.make_async_copy(w_refs[i].at[own_block(w)], w.old, mv_sem.at[i, 2]),
        )

    def to_pair(w, keep1, k):
        at = unit(w, keep1, k)
        return remote(w.g.at[(*at, 1 - core)], w.all.at[(*at, core)], send_sem.at[w.i, 0], pair_sem.at[w.i, 8 * keep1 + k], pair)

    def first(w, k):
        at = unit(w, 0, k)
        return remote(w.all.at[(*at, core)], w.first.at[k], send_sem.at[w.i, 1], s1_sem.at[w.i, k], w.to[0])

    def second(w, k):
        at = (k % 2, *w.block(1, 0, k // 2))
        return remote(w.all.at[(*at, core)], w.second.at[k], send_sem.at[w.i, 2], s2_sem.at[w.i, k], w.to[1])

    def third(w, k):
        at = (k, *w.block(1, 1, 0))
        return remote(w.all.at[(*at, core)], w.third.at[k], third_sem.at[w.i, k], s3_sem.at[w.i, k], w.to[2])

    def tell(w, stage):
        pl.semaphore_signal(free_sem.at[w.i, stage], inc=1, device_id={"dp": w.to[stage]}, device_id_type=MESH)

    def told(w, stage):
        pl.semaphore_wait(free_sem.at[w.i, stage], 1)

    def gather3(w, k):
        at = (k, *w.block(1, 1, 1), core)
        return remote(w.all.at[at], w.all.at[at], send_sem.at[w.i, 4], a3_sem.at[w.i, k], w.to[2])

    def gather2(w, k):
        at = (k % 2, *w.block(1, 1, 1 - k // 2), core)
        return remote(w.all.at[at], w.all.at[at], send_sem.at[w.i, 5], a2_sem.at[w.i, k], w.to[1])

    def gather1(w, k):
        at = (k % 2, *w.block(1, 1 - k // 4, 1 - (k // 2) % 2), core)
        return remote(w.all.at[at], w.all.at[at], send_sem.at[w.i, 6], a1_sem.at[w.i, k], w.to[0])

    def gather0(w, keep1, k):
        at = (k % 2, *w.block(keep1, 1 - k // 4, 1 - (k // 2) % 2), core)
        return remote(w.all.at[at], w.all.at[at], send_sem.at[w.i, 7], a0_sem.at[w.i], pair)

    def total(w, at, rows, *others):
        sum_ = w.all[(*at, core, rows, slice(None))].astype(F32) + w.all[(*at, 1 - core, rows, slice(None))].astype(F32)
        for other, k in others:
            sum_ = sum_ + other[k, rows, :].astype(F32)
        return sum_

    def add(w, at, *others):
        @pl.loop(0, w.old.shape[1] // SLAB)
        def _(r):
            rows = pl.ds(pl.multiple_of(r * SLAB, SLAB), SLAB)
            w.all[(*at, core, rows, slice(None))] = total(w, at, rows, *others).astype(BF16)

    def each(n, body):
        @pl.loop(0, n)
        def _(k):
            body(k)

    def start_loads(k):
        for w in weights:
            load(w, k).start()

    each(8, start_loads)

    barrier = pltpu.get_barrier_semaphore()
    for device in (pair, *partners):
        pl.semaphore_signal(barrier, inc=1, device_id={"dp": device}, device_id_type=MESH)
    pl.semaphore_wait(barrier, 4)

    for keep1 in (0, 1):

        def start_pair(k, keep1=keep1):
            for w in weights:
                to_pair(w, keep1, k).start()

        each(8, start_pair)
    for w in weights:
        load_rest(w).start()
    for w in weights:
        for copy in moments(w):
            copy.start()

    def stage1(k):
        for w in weights:
            load(w, k).wait()
            to_pair(w, 0, k).wait_recv()
            add(w, unit(w, 0, k))
        for w in weights:
            first(w, k).start()

    each(8, stage1)
    for w in weights:
        load_rest(w).wait()

    def stage2(k):
        for w in weights:
            to_pair(w, 1, k).wait_recv()
            first(w, k).wait_recv()
            add(w, unit(w, 1, k), (w.first, k))
        for w in weights:
            second(w, k).start()

    each(4, stage2)

    def stage3(k):
        for w in weights:
            to_pair(w, 1, 4 + k).wait_recv()
            first(w, 4 + k).wait_recv()
            second(w, k).wait_recv()
            add(w, unit(w, 1, 4 + k), (w.first, 4 + k), (w.second, k))
        for w in weights:
            third(w, k).start()

    each(2, stage3)
    for w in weights:
        for copy in moments(w):
            copy.wait()
        remote(w.first, w.first, send_sem.at[w.i, 1], s1_sem.at[w.i, 0], pair).wait_send()
        tell(w, 0)
        remote(w.second, w.second, send_sem.at[w.i, 2], s2_sem.at[w.i, 0], pair).wait_send()
        tell(w, 1)

    def update(k):
        for w in weights:
            to_pair(w, 1, 6 + k).wait_recv()
            first(w, 6 + k).wait_recv()
            second(w, 2 + k).wait_recv()
            third(w, k).wait()
            tell(w, 2)
            at = (k, *w.block(1, 1, 1))

            @pl.loop(0, w.old.shape[1] // SLAB)
            def _(r, w=w, at=at):
                rows = pl.ds(pl.multiple_of(r * SLAB, SLAB), SLAB)
                g = total(w, at, rows, (w.first, 6 + k), (w.second, 2 + k), (w.third, k)).astype(BF16).astype(F32)
                new, m, v = adamw(w.old[k, rows, :].astype(F32), w.m[k, rows, :], w.v[k, rows, :], g)
                w.m[k, rows, :] = m
                w.v[k, rows, :] = v
                w.all[(*at, core, rows, slice(None))] = new

        for w in weights:
            told(w, 2)
            gather3(w, k).start()

    each(2, update)

    def own21(k):
        for w in weights:
            gather2(w, k).start()
        for w in weights:
            gather1(w, k).start()

    for w in weights:
        told(w, 1)
        told(w, 0)
    each(2, own21)

    pl.semaphore_signal(read_sem, inc=1, device_id={"dp": pair}, device_id_type=MESH)
    pl.semaphore_wait(read_sem, 1)

    def own(k):
        for w in weights:
            gather0(w, 1, k).start()

    each(2, own)

    def back3(k):
        for w in weights:
            gather3(w, k).wait_recv()
            gather2(w, 2 + k).start()
        for w in weights:
            gather1(w, 2 + k).start()
            gather0(w, 1, 2 + k).start()

    each(2, back3)

    def back2(k):
        for w in weights:
            gather2(w, k).wait_recv()
            gather1(w, 4 + k).start()
            gather0(w, 1, 4 + k).start()

    each(4, back2)

    def back1(k):
        for w in weights:
            gather1(w, k).wait_recv()
            gather0(w, 0, k).start()

    each(8, back1)

    for w in weights:
        theirs = w.all.at[:, :, :, :, 1 - core]
        remote(theirs, theirs, send_sem.at[w.i, 7], a0_sem.at[w.i], pair).wait_recv()
    for w in weights:
        mine = w.all.at[:, :, :, :, core]
        for n, ref in ((0, mine), (4, w.third), (5, w.second), (6, w.first), (7, mine)):
            remote(ref, ref, send_sem.at[w.i, n], a0_sem.at[w.i], pair).wait_send()


def put(*refs):
    sem = refs[-1]
    copies = [
        pltpu.make_async_copy(refs[i].at[k], refs[9 + i].at[k], sem.at[i, k]) for i in range(9) for k in range(LAYERS)
    ]
    for copy in copies:
        copy.start()
    for copy in copies:
        copy.wait()


def solution(mesh):
    def step(*arrays):
        shapes = [a.shape[1:] for a in arrays[6:9]]

        def cut(a, i):
            return a.reshape(LAYERS, 2, 2, 2, 2, *shapes[i])

        operands = [cut(a, n % 3) for n, a in enumerate(arrays[:6])] + list(arrays[6:])
        blocks = [(n, rows, columns) for n in (8, 4, 2, LAYERS) for rows, columns in shapes]
        outs = pl.pallas_call(
            kernel,
            out_shape=[pltpu.VMEM((LAYERS, 2, 2, 2, 2, *s), BF16) for s in shapes] + [pltpu.VMEM((LAYERS, *s), F32) for s in shapes] * 2,
            in_specs=[pl.BlockSpec(memory_space=pl.ANY)] * 12,
            out_specs=[pl.BlockSpec(memory_space=pltpu.VMEM)] * 9,
            scratch_shapes=[
                *(pltpu.VMEM(s, BF16) for s in blocks),
                pltpu.SemaphoreType.DMA((3, 8)),
                pltpu.SemaphoreType.DMA((3,)),
                pltpu.SemaphoreType.DMA((3, 3)),
                pltpu.SemaphoreType.DMA((3, 16)),
                pltpu.SemaphoreType.DMA((3, 8)),
                pltpu.SemaphoreType.DMA((3, 4)),
                pltpu.SemaphoreType.DMA((3, 2)),
                pltpu.SemaphoreType.DMA((3, 2)),
                pltpu.SemaphoreType.DMA((3, 4)),
                pltpu.SemaphoreType.DMA((3, 8)),
                pltpu.SemaphoreType.DMA((3,)),
                pltpu.SemaphoreType.DMA((3, 8)),
                pltpu.SemaphoreType.DMA((3, 2)),
                pltpu.SemaphoreType.REGULAR((3, 3)),
                pltpu.SemaphoreType.REGULAR,
            ],
            compiler_params=pltpu.CompilerParams(collective_id=0, has_side_effects=True, vmem_limit_bytes=17 * 1024 * 1024),
            name="step",
        )(*operands)
        outs = [pltpu.with_memory_space_constraint(o, pltpu.VMEM) for o in outs]
        done = pl.pallas_call(
            put,
            out_shape=[jax.ShapeDtypeStruct(o.shape, o.dtype) for o in outs],
            in_specs=[pl.BlockSpec(memory_space=pl.ANY)] * 9,
            out_specs=[pl.BlockSpec(memory_space=pl.ANY)] * 9,
            scratch_shapes=[pltpu.SemaphoreType.DMA((9, LAYERS))],
            compiler_params=pltpu.CompilerParams(vmem_limit_bytes=17 * 1024 * 1024),
            name="put",
        )(*outs)
        whole = [o.reshape(a.shape) for o, a in zip(done[:3], arrays[3:6], strict=True)]
        return (*whole, *done[3:])

    all_of, part = P(None, None, None), P(None, "dp", None)
    return jax.shard_map(
        step,
        mesh=mesh,
        in_specs=(P(("rep", "dp"), None, None, None),) * 3 + (all_of,) * 3 + (part,) * 6,
        out_specs=(P("rep", None, None),) * 3 + (P("rep", "dp", None),) * 6,
        check_vma=False,
    )
```

```python
import jax
import jax.numpy as jnp
from jax import lax
from jax.experimental import pallas as pl
from jax.experimental.pallas import tpu as pltpu
from jax.sharding import PartitionSpec as P

BF16, F32 = jnp.bfloat16, jnp.float32
MESH = pl.DeviceIdType.MESH
LAYERS = 2
ORDERS = ((0, 1, 2), (1, 2, 0), (2, 0, 1))
STRIDES = (8, 4, 2)
SLAB = 16
PARTS = (16, 16, 48)


def adamw(w, m, v, g):
    m = 0.9 * m + 0.1 * g
    v = 0.95 * v + 0.05 * g * g
    step = m * lax.rsqrt(v + 1e-8) + 0.1 * w
    return (w - 0.02 * step).astype(BF16), m, v


class Weight:
    def __init__(self, order, where, core, **refs):
        self.order, self.core = order, core
        self.mine = [where[axis] for axis in order]
        self.__dict__.update(refs)

    def place(self, *stages):
        xyz = [None] * 3
        for axis, coordinate in zip(self.order, stages, strict=True):
            xyz[axis] = coordinate
        return tuple(xyz)

    def block(self, keep1, keep2, keep3):
        return self.place(*(1 - m + k * (2 * m - 1) for m, k in zip(self.mine, (keep1, keep2, keep3), strict=True)))


def kernel(*refs):
    g_refs, w_refs, m_refs, v_refs = (refs[i : i + 3] for i in (0, 3, 6, 9))
    all_refs, m_outs, v_outs = (refs[i : i + 3] for i in (12, 15, 18))
    firsts, seconds, thirds, olds = (refs[i : i + 3] for i in (21, 24, 27, 30))
    load_sem, pair_sem, s1_sem, s2_sem, s3_sem, a3_sem, a2_sem, a1_sem, a0_sem, send_sem, third_sem, free_sem, read_sem = refs[33:]

    me = lax.axis_index("dp")
    core = me % 2
    where = [(me // s) % 2 for s in STRIDES]
    partners = [me + s * (1 - 2 * b) for s, b in zip(STRIDES, where, strict=True)]
    pair = me + 1 - 2 * core

    weights = [
        Weight(
            ORDERS[i], where, core, i=i, part=PARTS[i], rows=olds[i].shape[1], g=g_refs[i], all=all_refs[i], m=m_outs[i], v=v_outs[i],
            first=firsts[i], second=seconds[i], third=thirds[i], old=olds[i],
            to=[partners[axis] for axis in ORDERS[i]],
        )
        for i in range(3)
    ]

    def remote(src, dst, send, recv, device):
        return pltpu.make_async_remote_copy(
            src_ref=src, dst_ref=dst, send_sem=send, recv_sem=recv, device_id={"dp": device}, device_id_type=MESH
        )

    def sent(w, n, like):
        remote(like, like, send_sem.at[w.i, n], a0_sem.at[w.i], pair).wait_send()

    def received(w, sem, like):
        remote(like, like, send_sem.at[w.i, 0], sem, pair).wait_recv()

    def unit(w, keep1, k):
        return (k % 2, *w.block(keep1, k // 4, (k // 2) % 2))

    def stage(w):
        return pltpu.make_async_copy(w.g.at[(slice(None), *w.block(0, 0, 0), 1 - core)], w.old, load_sem.at[w.i, 0])

    def load(w, keep2):
        at = (slice(None), *w.place(1 - w.mine[0], 1 - w.mine[1] + keep2 * (2 * w.mine[1] - 1), slice(None)), core)
        return pltpu.make_async_copy(w.g.at[at], w.all.at[at], load_sem.at[w.i, 1 + keep2])

    def load_rest(w):
        at = (slice(None), *w.place(w.mine[0], slice(None), slice(None)), core)
        return pltpu.make_async_copy(w.g.at[at], w.all.at[at], load_sem.at[w.i, 3])

    def load_m(w):
        return pltpu.make_async_copy(m_refs[w.i], w.m, load_sem.at[w.i, 4])

    def load_v(w):
        return pltpu.make_async_copy(v_refs[w.i], w.v, load_sem.at[w.i, 5])

    def load_w(w):
        return pltpu.make_async_copy(w_refs[w.i].at[(slice(None), *w.block(1, 1, 1), core)], w.old, load_sem.at[w.i, 6])

    def to_pair(w, keep1, k, recv):
        at = unit(w, keep1, k)
        return remote(w.g.at[(*at, 1 - core)], w.all.at[(*at, core)], send_sem.at[w.i, 0], pair_sem.at[w.i, recv], pair)

    def staged_to_pair(w, k, lo, n, recv):
        rows = pl.ds(lo, n)
        return remote(
            w.old.at[k, rows], w.all.at[(*unit(w, 0, k), core, rows)], send_sem.at[w.i, 0], pair_sem.at[w.i, recv], pair
        )

    def first(w, k, lo=0, n=None):
        rows = pl.ds(lo, w.rows if n is None else n)
        at = (*unit(w, 0, k), core, rows)
        return remote(w.all.at[at], w.first.at[k, rows], send_sem.at[w.i, 1], s1_sem.at[w.i, k // 2], w.to[0])

    def second(w, k):
        at = (k % 2, *w.block(1, 0, k // 2))
        return remote(w.all.at[(*at, core)], w.second.at[k], send_sem.at[w.i, 2], s2_sem.at[w.i, k // 2], w.to[1])

    def third(w, k):
        at = (k, *w.block(1, 1, 0))
        return remote(w.all.at[(*at, core)], w.third.at[k], third_sem.at[w.i, k], s3_sem.at[w.i, k], w.to[2])

    def tell(w, stage):
        pl.semaphore_signal(free_sem.at[w.i, stage], inc=1, device_id={"dp": w.to[stage]}, device_id_type=MESH)

    def told(w, stage):
        pl.semaphore_wait(free_sem.at[w.i, stage], 1)

    def gather3(w, k):
        at = (k, *w.block(1, 1, 1), core)
        return remote(w.all.at[at], w.all.at[at], send_sem.at[w.i, 3], a3_sem.at[w.i], w.to[2])

    def gather2(w, k):
        at = (k % 2, *w.block(1, 1, 1 - k // 2), core)
        return remote(w.all.at[at], w.all.at[at], send_sem.at[w.i, 4], a2_sem.at[w.i, k // 2], w.to[1])

    def came(w, keep1, k, lo, n):
        return (k % 2, *w.block(keep1, 1 - k // 4, 1 - (k // 2) % 2), core, pl.ds(lo, w.rows if n is None else n))

    def gather1(w, k, recv, lo=0, n=None):
        at = came(w, 1, k, lo, n)
        return remote(w.all.at[at], w.all.at[at], send_sem.at[w.i, 5], a1_sem.at[w.i, recv], w.to[0])

    def gather0(w, keep1, k, lo=0, n=None):
        at = came(w, keep1, k, lo, n)
        return remote(w.all.at[at], w.all.at[at], send_sem.at[w.i, 6], a0_sem.at[w.i], pair)

    def total(w, at, rows, *others):
        sum_ = w.all[(*at, core, rows, slice(None))].astype(F32) + w.all[(*at, 1 - core, rows, slice(None))].astype(F32)
        for other, k in others:
            sum_ = sum_ + other[k, rows, :].astype(F32)
        return sum_

    def slabs(lo, n, body):
        @pl.loop(0, n // SLAB)
        def _(r):
            body(pl.ds(pl.multiple_of(lo + r * SLAB, SLAB), SLAB))

    def add(w, at, *others, lo=0, n=None):
        def body(rows):
            w.all[(*at, core, rows, slice(None))] = total(w, at, rows, *others).astype(BF16)

        slabs(lo, w.rows if n is None else n, body)

    def each(lo, hi, body):
        @pl.loop(lo, hi)
        def _(k):
            body(k)

    for w in weights:
        stage(w).start()
    for keep2 in (0, 1):
        for w in weights:
            load(w, keep2).start()

    barrier = pltpu.get_barrier_semaphore()
    for device in (pair, *partners):
        pl.semaphore_signal(barrier, inc=1, device_id={"dp": device}, device_id_type=MESH)
    for w in weights:
        stage(w).wait()
    pl.semaphore_wait(barrier, 4)

    for w in weights:
        staged_to_pair(w, 0, 0, w.part, 0).start()
    for w in weights:
        staged_to_pair(w, 0, w.part, w.rows - w.part, 1).start()
    for w in weights:
        staged_to_pair(w, 1, 0, w.rows, 2).start()

    def start_pair(k):
        for w in weights:
            to_pair(w, 0, k, 3).start()

    each(2, 8, start_pair)

    def start_pair_rest(k):
        for w in weights:
            to_pair(w, 1, k, 4).start()

    each(0, 8, start_pair_rest)
    for w in weights:
        load_rest(w).start()

    for w in weights:
        load(w, 0).wait()
    for recv, k, begin, end in ((0, 0, 0, 1), (1, 0, 1, 2), (2, 1, 0, 2)):
        for w in weights:
            edges = (0, w.part, w.rows)
            lo, n = edges[begin], edges[end] - edges[begin]
            received(w, pair_sem.at[w.i, recv], w.old.at[0, pl.ds(0, n)])
            add(w, unit(w, 0, k), lo=lo, n=n)
            first(w, k, lo, n).start()
    for w in weights:
        load(w, 1).wait()
        received(w, pair_sem.at[w.i, 3], w.first.at[pl.ds(0, 6)])

    def stage1(k):
        for w in weights:
            add(w, unit(w, 0, k))
        for w in weights:
            first(w, k).start()

    each(2, 8, stage1)
    for w in weights:
        load_m(w).start()
        load_v(w).start()
        load_rest(w).wait()
        received(w, pair_sem.at[w.i, 4], w.first)
        sent(w, 0, w.all.at[:, :, :, :, core])
        load_w(w).start()

    def stage2(k):
        for w in weights:
            add(w, unit(w, 1, k), (w.first, k))
        for w in weights:
            second(w, k).start()

    for n in (0, 1):
        for w in weights:
            received(w, s1_sem.at[w.i, n], w.third)
        each(2 * n, 2 * n + 2, stage2)

    def stage3(k):
        for w in weights:
            add(w, unit(w, 1, 4 + k), (w.first, 4 + k), (w.second, k))
        for w in weights:
            third(w, k).start()

    for w in weights:
        received(w, s1_sem.at[w.i, 2], w.third)
        received(w, s2_sem.at[w.i, 0], w.third)
    each(0, 2, stage3)
    for w in weights:
        load_m(w).wait()
        load_v(w).wait()
        load_w(w).wait()
        sent(w, 1, w.first)
        tell(w, 0)
        received(w, s1_sem.at[w.i, 3], w.third)
        sent(w, 2, w.second)
        tell(w, 1)
        received(w, s2_sem.at[w.i, 1], w.third)

    def update(k):
        for w in weights:
            third(w, k).wait()
            tell(w, 2)
            at = (k, *w.block(1, 1, 1))

            def body(rows, w=w, at=at):
                g = total(w, at, rows, (w.first, 6 + k), (w.second, 2 + k), (w.third, k)).astype(BF16).astype(F32)
                new, m, v = adamw(w.old[k, rows, :].astype(F32), w.m[k, rows, :], w.v[k, rows, :], g)
                w.m[k, rows, :] = m
                w.v[k, rows, :] = v
                w.all[(*at, core, rows, slice(None))] = new

            slabs(0, w.rows, body)

        for w in weights:
            told(w, 2)
            gather3(w, k).start()

    each(0, 2, update)

    def own21(k):
        for w in weights:
            gather2(w, k).start()
        for w in weights:
            gather1(w, k, 0).start()

    for w in weights:
        told(w, 1)
        told(w, 0)
    each(0, 2, own21)

    pl.semaphore_signal(read_sem, inc=1, device_id={"dp": pair}, device_id_type=MESH)
    pl.semaphore_wait(read_sem, 1)

    def own0(k):
        for w in weights:
            gather0(w, 1, k).start()

    each(0, 2, own0)

    def back3(k):
        for w in weights:
            gather2(w, 2 + k).start()
        for w in weights:
            gather1(w, 2 + k, 1).start()
            gather0(w, 1, 2 + k).start()

    for w in weights:
        received(w, a3_sem.at[w.i], w.third)
    each(0, 2, back3)

    def back2(k):
        for w in weights:
            gather1(w, k, 2).start()
            gather0(w, 1, k).start()

    for w in weights:
        received(w, a2_sem.at[w.i, 0], w.third)
    each(4, 6, back2)
    for w in weights:
        received(w, a2_sem.at[w.i, 1], w.third)
        gather1(w, 6, 3).start()
    for w in weights:
        gather1(w, 7, 4, 0, w.rows - w.part).start()
    for w in weights:
        gather1(w, 7, 5, w.rows - w.part, w.part).start()
    for k in (6, 7):
        for w in weights:
            gather0(w, 1, k).start()

    def back1(k):
        for w in weights:
            gather0(w, 0, k).start()

    for n in (0, 1, 2):
        for w in weights:
            received(w, a1_sem.at[w.i, n], w.third)
        each(2 * n, 2 * n + 2, back1)
    for w in weights:
        received(w, a1_sem.at[w.i, 3], w.third.at[0])
        gather0(w, 0, 6).start()
    for w in weights:
        received(w, a1_sem.at[w.i, 4], w.third.at[0, pl.ds(0, w.rows - w.part)])
        gather0(w, 0, 7, 0, w.rows - w.part).start()
    for w in weights:
        received(w, a1_sem.at[w.i, 5], w.third.at[0, pl.ds(0, w.part)])
        gather0(w, 0, 7, w.rows - w.part, w.part).start()

    for w in weights:
        for n, like in ((3, w.third), (4, w.second), (5, w.first)):
            sent(w, n, like)
    for w in weights:
        received(w, a0_sem.at[w.i], w.all.at[:, :, :, :, 1 - core])
        sent(w, 6, w.all.at[:, :, :, :, core])


def put(*refs):
    sem = refs[-1]
    copies = [
        pltpu.make_async_copy(refs[i].at[k], refs[9 + i].at[k], sem.at[i, k]) for i in range(9) for k in range(LAYERS)
    ]
    for copy in copies:
        copy.start()
    for copy in copies:
        copy.wait()


def solution(mesh):
    def step(*arrays):
        shapes = [a.shape[1:] for a in arrays[6:9]]

        def cut(a, i):
            return a.reshape(LAYERS, 2, 2, 2, 2, *shapes[i])

        operands = [cut(a, n % 3) for n, a in enumerate(arrays[:6])] + list(arrays[6:])
        blocks = [(n, rows, columns) for n in (8, 4, 2, LAYERS) for rows, columns in shapes]
        outs = pl.pallas_call(
            kernel,
            out_shape=[pltpu.VMEM((LAYERS, 2, 2, 2, 2, *s), BF16) for s in shapes] + [pltpu.VMEM((LAYERS, *s), F32) for s in shapes] * 2,
            in_specs=[pl.BlockSpec(memory_space=pl.ANY)] * 12,
            out_specs=[pl.BlockSpec(memory_space=pltpu.VMEM)] * 9,
            scratch_shapes=[
                *(pltpu.VMEM(s, BF16) for s in blocks),
                *(pltpu.SemaphoreType.DMA((3, n)) for n in (7, 5, 4, 2, 2)),
                pltpu.SemaphoreType.DMA((3,)),
                *(pltpu.SemaphoreType.DMA((3, n)) for n in (2, 6)),
                pltpu.SemaphoreType.DMA((3,)),
                *(pltpu.SemaphoreType.DMA((3, n)) for n in (7, 2)),
                pltpu.SemaphoreType.REGULAR((3, 3)),
                pltpu.SemaphoreType.REGULAR,
            ],
            compiler_params=pltpu.CompilerParams(collective_id=0, has_side_effects=True, vmem_limit_bytes=17 * 1024 * 1024),
            name="step",
        )(*operands)
        outs = [pltpu.with_memory_space_constraint(o, pltpu.VMEM) for o in outs]
        done = pl.pallas_call(
            put,
            out_shape=[jax.ShapeDtypeStruct(o.shape, o.dtype) for o in outs],
            in_specs=[pl.BlockSpec(memory_space=pl.ANY)] * 9,
            out_specs=[pl.BlockSpec(memory_space=pl.ANY)] * 9,
            scratch_shapes=[pltpu.SemaphoreType.DMA((9, LAYERS))],
            compiler_params=pltpu.CompilerParams(vmem_limit_bytes=17 * 1024 * 1024),
            name="put",
        )(*outs)
        whole = [o.reshape(a.shape) for o, a in zip(done[:3], arrays[3:6], strict=True)]
        return (*whole, *done[3:])

    all_of, part = P(None, None, None), P(None, "dp", None)
    return jax.shard_map(
        step,
        mesh=mesh,
        in_specs=(P(("rep", "dp"), None, None, None),) * 3 + (all_of,) * 3 + (part,) * 6,
        out_specs=(P("rep", None, None),) * 3 + (P("rep", "dp", None),) * 6,
        check_vma=False,
    )
```

```python
import jax
import jax.numpy as jnp
from jax import lax
from jax.experimental import pallas as pl
from jax.experimental.pallas import tpu as pltpu
from jax.sharding import PartitionSpec as P

BF16, F32 = jnp.bfloat16, jnp.float32
MESH = pl.DeviceIdType.MESH
LAYERS = 2
ORDERS = ((0, 1, 2), (1, 2, 0), (2, 0, 1))
STRIDES = (8, 4, 2)
SLAB = 16
PARTS = (16, 16, 48)
PUT_FLOPS = 200_000_000


def adamw(w, m, v, g):
    m = 0.9 * m + 0.1 * g
    v = 0.95 * v + 0.05 * g * g
    step = m * lax.rsqrt(v + 1e-8) + 0.1 * w
    return (w - 0.02 * step).astype(BF16), m, v


class Weight:
    def __init__(self, order, where, core, **refs):
        self.order, self.core = order, core
        self.mine = [where[axis] for axis in order]
        self.__dict__.update(refs)

    def place(self, *stages):
        xyz = [None] * 3
        for axis, coordinate in zip(self.order, stages, strict=True):
            xyz[axis] = coordinate
        return tuple(xyz)

    def block(self, keep1, keep2, keep3):
        return self.place(*(1 - m + k * (2 * m - 1) for m, k in zip(self.mine, (keep1, keep2, keep3), strict=True)))


def kernel(*refs):
    g_refs, w_refs, m_refs, v_refs = (refs[i : i + 3] for i in (0, 3, 6, 9))
    all_refs, m_outs, v_outs, late_refs = (refs[i : i + 3] for i in (12, 15, 18, 21))
    firsts, seconds, thirds, olds = (refs[i : i + 3] for i in (24, 27, 30, 33))
    load_sem, pair_sem, s1_sem, s2_sem, s3_sem, a3_sem, a2_sem, a1_sem, a0_sem, send_sem, third_sem, free_sem, read_sem = refs[36:]

    me = lax.axis_index("dp")
    core = me % 2
    where = [(me // s) % 2 for s in STRIDES]
    partners = [me + s * (1 - 2 * b) for s, b in zip(STRIDES, where, strict=True)]
    pair = me + 1 - 2 * core

    weights = [
        Weight(
            ORDERS[i], where, core, i=i, part=PARTS[i], rows=olds[i].shape[1], g=g_refs[i], all=all_refs[i], m=m_outs[i], v=v_outs[i],
            first=firsts[i], second=seconds[i], third=thirds[i], old=olds[i], late=late_refs[i],
            to=[partners[axis] for axis in ORDERS[i]],
        )
        for i in range(3)
    ]

    def remote(src, dst, send, recv, device):
        return pltpu.make_async_remote_copy(
            src_ref=src, dst_ref=dst, send_sem=send, recv_sem=recv, device_id={"dp": device}, device_id_type=MESH
        )

    def sent(w, n, like):
        remote(like, like, send_sem.at[w.i, n], a0_sem.at[w.i, 0], pair).wait_send()

    def received(w, sem, like):
        remote(like, like, send_sem.at[w.i, 0], sem, pair).wait_recv()

    def unit(w, keep1, k):
        return (k % 2, *w.block(keep1, k // 4, (k // 2) % 2))

    def stage(w):
        return pltpu.make_async_copy(w.g.at[(slice(None), *w.block(0, 0, 0), 1 - core)], w.old, load_sem.at[w.i, 0])

    def load(w, keep2):
        at = (slice(None), *w.place(1 - w.mine[0], 1 - w.mine[1] + keep2 * (2 * w.mine[1] - 1), slice(None)), core)
        return pltpu.make_async_copy(w.g.at[at], w.all.at[at], load_sem.at[w.i, 1 + keep2])

    def load_rest(w):
        at = (slice(None), *w.place(w.mine[0], slice(None), slice(None)), core)
        return pltpu.make_async_copy(w.g.at[at], w.all.at[at], load_sem.at[w.i, 3])

    def load_m(w):
        return pltpu.make_async_copy(m_refs[w.i], w.m, load_sem.at[w.i, 4])

    def load_v(w):
        return pltpu.make_async_copy(v_refs[w.i], w.v, load_sem.at[w.i, 5])

    def load_w(w):
        return pltpu.make_async_copy(w_refs[w.i].at[(slice(None), *w.block(1, 1, 1), core)], w.old, load_sem.at[w.i, 6])

    def to_pair(w, keep1, k, recv):
        at = unit(w, keep1, k)
        return remote(w.g.at[(*at, 1 - core)], w.all.at[(*at, core)], send_sem.at[w.i, 0], pair_sem.at[w.i, recv], pair)

    def staged_to_pair(w, k, lo, n, recv):
        rows = pl.ds(lo, n)
        return remote(
            w.old.at[k, rows], w.all.at[(*unit(w, 0, k), core, rows)], send_sem.at[w.i, 0], pair_sem.at[w.i, recv], pair
        )

    def first(w, k, lo=0, n=None):
        rows = pl.ds(lo, w.rows if n is None else n)
        at = (*unit(w, 0, k), core, rows)
        return remote(w.all.at[at], w.first.at[k, rows], send_sem.at[w.i, 1], s1_sem.at[w.i, k // 2], w.to[0])

    def second(w, k):
        at = (k % 2, *w.block(1, 0, k // 2))
        return remote(w.all.at[(*at, core)], w.second.at[k], send_sem.at[w.i, 2], s2_sem.at[w.i, k // 2], w.to[1])

    def third(w, k):
        at = (k, *w.block(1, 1, 0))
        return remote(w.all.at[(*at, core)], w.third.at[k], third_sem.at[w.i, k], s3_sem.at[w.i, k], w.to[2])

    def tell(w, stage):
        pl.semaphore_signal(free_sem.at[w.i, stage], inc=1, device_id={"dp": w.to[stage]}, device_id_type=MESH)

    def told(w, stage):
        pl.semaphore_wait(free_sem.at[w.i, stage], 1)

    def gather3(w, k):
        at = (k, *w.block(1, 1, 1), core)
        return remote(w.all.at[at], w.all.at[at], send_sem.at[w.i, 3], a3_sem.at[w.i], w.to[2])

    def gather2(w, k):
        at = (k % 2, *w.block(1, 1, 1 - k // 2), core)
        return remote(w.all.at[at], w.all.at[at], send_sem.at[w.i, 4], a2_sem.at[w.i, k // 2], w.to[1])

    def came(w, keep1, k, lo, n):
        return (k % 2, *w.block(keep1, 1 - k // 4, 1 - (k // 2) % 2), core, pl.ds(lo, w.rows if n is None else n))

    def gather1(w, k, recv, lo=0, n=None):
        at = came(w, 1, k, lo, n)
        return remote(w.all.at[at], w.all.at[at], send_sem.at[w.i, 5], a1_sem.at[w.i, recv], w.to[0])

    def gather0(w, keep1, k, lo=0, n=None):
        at = came(w, keep1, k, lo, n)
        return remote(w.all.at[at], w.all.at[at], send_sem.at[w.i, 6 + keep1], a0_sem.at[w.i, keep1], pair)

    def keep_late(w):
        at = (slice(None), *w.block(1, 0, 0), core)
        return pltpu.make_async_copy(w.all.at[at], w.late, load_sem.at[w.i, 0])

    def total(w, at, rows, *others):
        sum_ = w.all[(*at, core, rows, slice(None))].astype(F32) + w.all[(*at, 1 - core, rows, slice(None))].astype(F32)
        for other, k in others:
            sum_ = sum_ + other[k, rows, :].astype(F32)
        return sum_

    def slabs(lo, n, body):
        @pl.loop(0, n // SLAB)
        def _(r):
            body(pl.ds(pl.multiple_of(lo + r * SLAB, SLAB), SLAB))

    def add(w, at, *others, lo=0, n=None):
        def body(rows):
            w.all[(*at, core, rows, slice(None))] = total(w, at, rows, *others).astype(BF16)

        slabs(lo, w.rows if n is None else n, body)

    def each(lo, hi, body):
        @pl.loop(lo, hi)
        def _(k):
            body(k)

    for w in weights:
        stage(w).start()
    for keep2 in (0, 1):
        for w in weights:
            load(w, keep2).start()

    barrier = pltpu.get_barrier_semaphore()
    for device in (pair, *partners):
        pl.semaphore_signal(barrier, inc=1, device_id={"dp": device}, device_id_type=MESH)
    for w in weights:
        stage(w).wait()
    pl.semaphore_wait(barrier, 4)

    for w in weights:
        staged_to_pair(w, 0, 0, w.part, 0).start()
    for w in weights:
        staged_to_pair(w, 0, w.part, w.rows - w.part, 1).start()
    for w in weights:
        staged_to_pair(w, 1, 0, w.rows, 2).start()

    def start_pair(k):
        for w in weights:
            to_pair(w, 0, k, 3).start()

    each(2, 8, start_pair)

    def start_pair_rest(k):
        for w in weights:
            to_pair(w, 1, k, 4).start()

    each(0, 8, start_pair_rest)
    for w in weights:
        load_rest(w).start()

    for w in weights:
        load(w, 0).wait()
    for recv, k, begin, end in ((0, 0, 0, 1), (1, 0, 1, 2), (2, 1, 0, 2)):
        for w in weights:
            edges = (0, w.part, w.rows)
            lo, n = edges[begin], edges[end] - edges[begin]
            received(w, pair_sem.at[w.i, recv], w.old.at[0, pl.ds(0, n)])
            add(w, unit(w, 0, k), lo=lo, n=n)
            first(w, k, lo, n).start()
    for w in weights:
        load(w, 1).wait()
        received(w, pair_sem.at[w.i, 3], w.first.at[pl.ds(0, 6)])

    def stage1(k):
        for w in weights:
            add(w, unit(w, 0, k))
        for w in weights:
            first(w, k).start()

    each(2, 8, stage1)
    for w in weights:
        load_m(w).start()
        load_v(w).start()
        load_rest(w).wait()
        received(w, pair_sem.at[w.i, 4], w.first)
        sent(w, 0, w.all.at[:, :, :, :, core])
        load_w(w).start()

    def stage2(k):
        for w in weights:
            add(w, unit(w, 1, k), (w.first, k))
        for w in weights:
            second(w, k).start()

    for n in (0, 1):
        for w in weights:
            received(w, s1_sem.at[w.i, n], w.third)
        each(2 * n, 2 * n + 2, stage2)

    def stage3(k):
        for w in weights:
            add(w, unit(w, 1, 4 + k), (w.first, 4 + k), (w.second, k))
        for w in weights:
            third(w, k).start()

    for w in weights:
        received(w, s1_sem.at[w.i, 2], w.third)
        received(w, s2_sem.at[w.i, 0], w.third)
    each(0, 2, stage3)
    for w in weights:
        load_m(w).wait()
        load_v(w).wait()
        load_w(w).wait()
        sent(w, 1, w.first)
        tell(w, 0)
        received(w, s1_sem.at[w.i, 3], w.third)
        sent(w, 2, w.second)
        tell(w, 1)
        received(w, s2_sem.at[w.i, 1], w.third)

    def update(k):
        for w in weights:
            third(w, k).wait()
            tell(w, 2)
            at = (k, *w.block(1, 1, 1))

            def body(rows, w=w, at=at):
                g = total(w, at, rows, (w.first, 6 + k), (w.second, 2 + k), (w.third, k)).astype(BF16).astype(F32)
                new, m, v = adamw(w.old[k, rows, :].astype(F32), w.m[k, rows, :], w.v[k, rows, :], g)
                w.m[k, rows, :] = m
                w.v[k, rows, :] = v
                w.all[(*at, core, rows, slice(None))] = new

            slabs(0, w.rows, body)

        for w in weights:
            told(w, 2)
            gather3(w, k).start()

    each(0, 2, update)

    def own21(k):
        for w in weights:
            gather2(w, k).start()
        for w in weights:
            gather1(w, k, 0).start()

    for w in weights:
        told(w, 1)
        told(w, 0)
    each(0, 2, own21)

    pl.semaphore_signal(read_sem, inc=1, device_id={"dp": pair}, device_id_type=MESH)
    pl.semaphore_wait(read_sem, 1)

    def own0(k):
        for w in weights:
            gather0(w, 1, k).start()

    each(0, 2, own0)

    def back3(k):
        for w in weights:
            gather2(w, 2 + k).start()
        for w in weights:
            gather1(w, 2 + k, 1).start()
            gather0(w, 1, 2 + k).start()

    for w in weights:
        received(w, a3_sem.at[w.i], w.third)
    each(0, 2, back3)

    def back2(k):
        for w in weights:
            gather0(w, 1, k).start()

    for w in weights:
        received(w, a2_sem.at[w.i, 0], w.third)
        gather1(w, 4, 2).start()
    for w in weights:
        gather1(w, 5, 3, 0, w.rows - w.part).start()
    for w in weights:
        gather1(w, 5, 4, w.rows - w.part, w.part).start()
    each(4, 6, back2)
    for w in weights:
        received(w, a2_sem.at[w.i, 1], w.third)
        keep_late(w).start()
    each(6, 8, back2)

    def back1(k):
        for w in weights:
            gather0(w, 0, k).start()

    for n in (0, 1):
        for w in weights:
            received(w, a1_sem.at[w.i, n], w.third)
        each(2 * n, 2 * n + 2, back1)
    for w in weights:
        received(w, a1_sem.at[w.i, 2], w.third.at[0])
        gather0(w, 0, 4).start()
    for w in weights:
        received(w, a1_sem.at[w.i, 3], w.third.at[0, pl.ds(0, w.rows - w.part)])
        gather0(w, 0, 5, 0, w.rows - w.part).start()
    for w in weights:
        received(w, a1_sem.at[w.i, 4], w.third.at[0, pl.ds(0, w.part)])
        gather0(w, 0, 5, w.rows - w.part, w.part).start()

    for w in weights:
        keep_late(w).wait()
        for n, like in ((3, w.third), (4, w.second), (5, w.first.at[pl.ds(0, 6)]), (7, w.first)):
            sent(w, n, like)
        received(w, a0_sem.at[w.i, 1], w.first)
    for w in weights:
        received(w, a0_sem.at[w.i, 0], w.first.at[pl.ds(0, 6)])
        sent(w, 6, w.first.at[pl.ds(0, 6)])


def put(*refs):
    sem = refs[-1]
    copies = [
        pltpu.make_async_copy(refs[i].at[k], refs[9 + i].at[k], sem.at[i, k]) for i in range(9) for k in range(LAYERS)
    ]
    for copy in copies:
        copy.start()
    for copy in copies:
        copy.wait()


def patch(*refs):
    lates, theirs, outs = (refs[i : i + 3] for i in (3, 6, 9))
    sem = refs[12]
    core = lax.axis_index("dp") % 2
    where = [(lax.axis_index("dp") // s) % 2 for s in STRIDES]
    copies = []
    for i in range(3):
        w = Weight(ORDERS[i], where, core)
        for n, (src, side) in enumerate(((lates[i], core), (theirs[i], 1 - core))):
            copies.append(pltpu.make_async_copy(src, outs[i].at[(slice(None), *w.block(0, 0, 0), side)], sem.at[i, n]))
    for copy in copies:
        copy.start()
    for copy in copies:
        copy.wait()


def solution(mesh):
    def step(*arrays):
        shapes = [a.shape[1:] for a in arrays[6:9]]

        def cut(a, i):
            return a.reshape(LAYERS, 2, 2, 2, 2, *shapes[i])

        operands = [cut(a, n % 3) for n, a in enumerate(arrays[:6])] + list(arrays[6:])
        blocks = [(n, rows, columns) for n in (8, 4, 2, LAYERS) for rows, columns in shapes]
        outs = pl.pallas_call(
            kernel,
            out_shape=[pltpu.VMEM((LAYERS, 2, 2, 2, 2, *s), BF16) for s in shapes] + [pltpu.VMEM((LAYERS, *s), F32) for s in shapes] * 2 + [jax.ShapeDtypeStruct((LAYERS, *s), BF16) for s in shapes],
            in_specs=[pl.BlockSpec(memory_space=pl.ANY)] * 12,
            out_specs=[pl.BlockSpec(memory_space=pltpu.VMEM)] * 9 + [pl.BlockSpec(memory_space=pl.ANY)] * 3,
            scratch_shapes=[
                *(pltpu.VMEM(s, BF16) for s in blocks),
                *(pltpu.SemaphoreType.DMA((3, n)) for n in (7, 5, 4, 2, 2)),
                pltpu.SemaphoreType.DMA((3,)),
                *(pltpu.SemaphoreType.DMA((3, n)) for n in (2, 5, 2, 8, 2)),
                pltpu.SemaphoreType.REGULAR((3, 3)),
                pltpu.SemaphoreType.REGULAR,
            ],
            compiler_params=pltpu.CompilerParams(collective_id=0, has_side_effects=True, vmem_limit_bytes=17 * 1024 * 1024),
            name="step",
        )(*operands)
        late = [lax.ppermute(o, "dp", [(d, d ^ STRIDES[order[0]]) for d in range(16)]) for o, order in zip(outs[9:], ORDERS, strict=True)]
        outs = [pltpu.with_memory_space_constraint(o, pltpu.VMEM) for o in outs[:9]]
        done = list(pl.pallas_call(
            put,
            out_shape=[jax.ShapeDtypeStruct(o.shape, o.dtype) for o in outs],
            in_specs=[pl.BlockSpec(memory_space=pl.ANY)] * 9,
            out_specs=[pl.BlockSpec(memory_space=pl.ANY)] * 9,
            scratch_shapes=[pltpu.SemaphoreType.DMA((9, LAYERS))],
            compiler_params=pltpu.CompilerParams(vmem_limit_bytes=17 * 1024 * 1024),
            cost_estimate=pl.CostEstimate(flops=PUT_FLOPS, bytes_accessed=2 * 43_000_000, transcendentals=0),
            name="put",
        )(*outs))
        for i in range(3):
            late[i], done[3 + i] = lax.optimization_barrier((late[i], done[3 + i]))
        theirs = [lax.ppermute(o, "dp", [(d, d ^ 1) for d in range(16)]) for o in late]
        patched = pl.pallas_call(
            patch,
            out_shape=[jax.ShapeDtypeStruct(o.shape, o.dtype) for o in done[:3]],
            in_specs=[pl.BlockSpec(memory_space=pl.ANY)] * 3 + [pl.BlockSpec(memory_space=pltpu.VMEM)] * 6,
            out_specs=[pl.BlockSpec(memory_space=pl.ANY)] * 3,
            input_output_aliases={0: 0, 1: 1, 2: 2},
            scratch_shapes=[
                pltpu.SemaphoreType.DMA((3, 2)),
            ],
            compiler_params=pltpu.CompilerParams(vmem_limit_bytes=17 * 1024 * 1024),
            name="patch",
        )(*done[:3], *(pltpu.with_memory_space_constraint(o, pltpu.VMEM) for o in (*late, *theirs)))
        done = [*patched, *done[3:]]
        whole = [o.reshape(a.shape) for o, a in zip(done[:3], arrays[3:6], strict=True)]
        return (*whole, *done[3:])

    all_of, part = P(None, None, None), P(None, "dp", None)
    return jax.shard_map(
        step,
        mesh=mesh,
        in_specs=(P(("rep", "dp"), None, None, None),) * 3 + (all_of,) * 3 + (part,) * 6,
        out_specs=(P("rep", None, None),) * 3 + (P("rep", "dp", None),) * 6,
        check_vma=False,
    )
```

```python
import functools

import jax
import jax.numpy as jnp
from jax import lax
from jax.experimental import pallas as pl
from jax.experimental.pallas import tpu as pltpu
from jax.sharding import PartitionSpec as P

BF16, F32 = jnp.bfloat16, jnp.float32
MESH = pl.DeviceIdType.MESH
LAYERS = 2
ORDERS = ((0, 1, 2), (1, 2, 0), (2, 0, 1))
STRIDES = (8, 4, 2)
SLAB = 16
PARTS = (16, 16, 48)
PUT_FLOPS = 200_000_000


def adamw(w, m, v, g):
    m = 0.9 * m + 0.1 * g
    v = 0.95 * v + 0.05 * g * g
    step = m * lax.rsqrt(v + 1e-8) + 0.1 * w
    return (w - 0.02 * step).astype(BF16), m, v


class Weight:
    def __init__(self, order, where, core, **refs):
        self.order, self.core = order, core
        self.mine = [where[axis] for axis in order]
        self.__dict__.update(refs)

    def place(self, *stages):
        xyz = [None] * 3
        for axis, coordinate in zip(self.order, stages, strict=True):
            xyz[axis] = coordinate
        return tuple(xyz)

    def block(self, keep1, keep2, keep3):
        return self.place(*(1 - m + k * (2 * m - 1) for m, k in zip(self.mine, (keep1, keep2, keep3), strict=True)))


def kernel(*refs):
    g_refs, w_refs, m_refs, v_refs = (refs[i : i + 3] for i in (0, 3, 6, 9))
    all_refs, m_outs, v_outs, late_refs = (refs[i : i + 3] for i in (12, 15, 18, 21))
    firsts, seconds, thirds, olds = (refs[i : i + 3] for i in (24, 27, 30, 33))
    load_sem, pair_sem, rest_sem, s1_sem, s2_sem, s3_sem, a3_sem, a2_sem, a1_sem, last_sem, own_sem, a0_sem, all_send, send_sem, third_sem, free_sem, third_free, read_sem = refs[36:]

    me = lax.axis_index("dp")
    core = me % 2
    where = [(me // s) % 2 for s in STRIDES]
    partners = [me + s * (1 - 2 * b) for s, b in zip(STRIDES, where, strict=True)]
    pair = me + 1 - 2 * core

    weights = [
        Weight(
            ORDERS[i], where, core, i=i, part=PARTS[i], rows=olds[i].shape[1], g=g_refs[i], all=all_refs[i], m=m_outs[i], v=v_outs[i],
            first=firsts[i], second=seconds[i], third=thirds[i], old=olds[i], late=late_refs[i],
            to=[partners[axis] for axis in ORDERS[i]],
        )
        for i in range(3)
    ]

    def remote(src, dst, send, recv, device):
        return pltpu.make_async_remote_copy(
            src_ref=src, dst_ref=dst, send_sem=send, recv_sem=recv, device_id={"dp": device}, device_id_type=MESH
        )

    gate = weights[0]
    like = {
        2: gate.third,
        6: gate.first.at[pl.ds(0, 6)],
        8: gate.first,
        12: gate.all.at[:, :, :, :, 0, pl.ds(0, 48)],
        16: gate.all.at[:, :, :, :, 0],
        24: gate.all.at[:, :, :, :, :, pl.ds(0, 48)],
    }

    def sent(sem, ref):
        remote(ref, ref, sem, own_sem, pair).wait_send()

    def received(sem, ref):
        remote(ref, ref, own_sem, sem, pair).wait_recv()

    def loaded(n, ref):
        pltpu.make_async_copy(ref, ref, load_sem.at[n]).wait()

    def unit(w, keep1, k):
        return (k % 2, *w.block(keep1, k // 4, (k // 2) % 2))

    def stage(w):
        return pltpu.make_async_copy(w.g.at[(slice(None), *w.block(0, 0, 0), 1 - core)], w.old, load_sem.at[0])

    def load(w, keep2):
        at = (slice(None), *w.place(1 - w.mine[0], 1 - w.mine[1] + keep2 * (2 * w.mine[1] - 1), slice(None)), core)
        return pltpu.make_async_copy(w.g.at[at], w.all.at[at], load_sem.at[1 + keep2])

    def load_rest(w):
        at = (slice(None), *w.place(w.mine[0], slice(None), slice(None)), core)
        return pltpu.make_async_copy(w.g.at[at], w.all.at[at], load_sem.at[3])

    def load_m(w):
        return pltpu.make_async_copy(m_refs[w.i], w.m, load_sem.at[4])

    def load_v(w):
        return pltpu.make_async_copy(v_refs[w.i], w.v, load_sem.at[5])

    def load_w(w):
        return pltpu.make_async_copy(w_refs[w.i].at[(slice(None), *w.block(1, 1, 1), core)], w.old, load_sem.at[6])

    def to_pair(w, keep1, k):
        at, recv = unit(w, keep1, k), rest_sem if keep1 else pair_sem.at[w.i, 3]
        return remote(w.g.at[(*at, 1 - core)], w.all.at[(*at, core)], send_sem.at[w.i, 0], recv, pair)

    def staged_to_pair(w, k, lo, n, recv):
        rows = pl.ds(lo, n)
        return remote(
            w.old.at[k, rows], w.all.at[(*unit(w, 0, k), core, rows)], send_sem.at[w.i, 0], pair_sem.at[w.i, recv], pair
        )

    def first(w, k, lo=0, n=None):
        rows = pl.ds(lo, w.rows if n is None else n)
        at = (*unit(w, 0, k), core, rows)
        return remote(w.all.at[at], w.first.at[k, rows], all_send.at[0], s1_sem.at[k // 2], w.to[0])

    def second(w, k):
        at = (k % 2, *w.block(1, 0, k // 2))
        return remote(w.all.at[(*at, core)], w.second.at[k], all_send.at[1], s2_sem.at[k // 2], w.to[1])

    def third(w, k):
        at = (k, *w.block(1, 1, 0))
        return remote(w.all.at[(*at, core)], w.third.at[k], third_sem.at[w.i, k], s3_sem.at[w.i, k], w.to[2])

    def tell(n, stage):
        for w in weights:
            pl.semaphore_signal(free_sem.at[n], inc=1, device_id={"dp": w.to[stage]}, device_id_type=MESH)

    def told(n):
        pl.semaphore_wait(free_sem.at[n], 3)

    def gather3(w, k):
        at = (k, *w.block(1, 1, 1), core)
        return remote(w.all.at[at], w.all.at[at], all_send.at[2], a3_sem, w.to[2])

    def gather2(w, k):
        at = (k % 2, *w.block(1, 1, 1 - k // 2), core)
        return remote(w.all.at[at], w.all.at[at], all_send.at[3], a2_sem.at[k // 2], w.to[1])

    def came(w, keep1, k, lo, n):
        return (k % 2, *w.block(keep1, 1 - k // 4, 1 - (k // 2) % 2), core, pl.ds(lo, w.rows if n is None else n))

    def gather1(w, k, recv, lo=0, n=None):
        at = came(w, 1, k, lo, n)
        sem = a1_sem.at[recv] if recv < 2 else last_sem.at[w.i, recv - 2]
        return remote(w.all.at[at], w.all.at[at], send_sem.at[w.i, 1], sem, w.to[0])

    def gather0(w, keep1, k, lo=0, n=None):
        at = came(w, keep1, k, lo, n)
        send, recv = (all_send.at[4], own_sem) if keep1 else (send_sem.at[w.i, 2], a0_sem.at[w.i])
        return remote(w.all.at[at], w.all.at[at], send, recv, pair)

    def keep_late(w):
        at = (slice(None), *w.block(1, 0, 0), core)
        return pltpu.make_async_copy(w.all.at[at], w.late, load_sem.at[0])

    def total(w, at, rows, *others):
        sum_ = w.all[(*at, core, rows, slice(None))].astype(F32) + w.all[(*at, 1 - core, rows, slice(None))].astype(F32)
        for other, k in others:
            sum_ = sum_ + other[k, rows, :].astype(F32)
        return sum_

    def slabs(lo, n, body):
        @pl.loop(0, n // SLAB)
        def _(r):
            body(pl.ds(pl.multiple_of(lo + r * SLAB, SLAB), SLAB))

    def add(w, at, *others, lo=0, n=None):
        def body(rows):
            w.all[(*at, core, rows, slice(None))] = total(w, at, rows, *others).astype(BF16)

        slabs(lo, w.rows if n is None else n, body)

    def each(lo, hi, body):
        @pl.loop(lo, hi)
        def _(k):
            body(k)

    for w in weights:
        stage(w).start()
    for keep2 in (0, 1):
        for w in weights:
            load(w, keep2).start()

    barrier = pltpu.get_barrier_semaphore()
    for device in (pair, *partners):
        pl.semaphore_signal(barrier, inc=1, device_id={"dp": device}, device_id_type=MESH)
    loaded(0, like[6])
    pl.semaphore_wait(barrier, 4)

    for w in weights:
        staged_to_pair(w, 0, 0, w.part, 0).start()
    for w in weights:
        staged_to_pair(w, 0, w.part, w.rows - w.part, 1).start()
    for w in weights:
        staged_to_pair(w, 1, 0, w.rows, 2).start()

    def start_pair(k):
        for w in weights:
            to_pair(w, 0, k).start()

    each(2, 8, start_pair)

    def start_pair_rest(k):
        for w in weights:
            to_pair(w, 1, k).start()

    each(0, 8, start_pair_rest)
    for w in weights:
        load_rest(w).start()

    loaded(1, like[12])
    for recv, k, begin, end in ((0, 0, 0, 1), (1, 0, 1, 2), (2, 1, 0, 2)):
        for w in weights:
            edges = (0, w.part, w.rows)
            lo, n = edges[begin], edges[end] - edges[begin]
            received(pair_sem.at[w.i, recv], w.old.at[0, pl.ds(0, n)])
            add(w, unit(w, 0, k), lo=lo, n=n)
            first(w, k, lo, n).start()
    loaded(2, like[12])
    for w in weights:
        received(pair_sem.at[w.i, 3], like[6])

    def stage1(k):
        for w in weights:
            add(w, unit(w, 0, k))
        for w in weights:
            first(w, k).start()

    each(2, 8, stage1)
    for w in weights:
        load_m(w).start()
        load_v(w).start()
    loaded(3, like[24])
    received(rest_sem, like[24])
    for w in weights:
        sent(send_sem.at[w.i, 0], like[16])
        load_w(w).start()

    def stage2(k):
        for w in weights:
            add(w, unit(w, 1, k), (w.first, k))
        for w in weights:
            second(w, k).start()

    for n in (0, 1):
        received(s1_sem.at[n], like[6])
        each(2 * n, 2 * n + 2, stage2)

    def stage3(k):
        for w in weights:
            add(w, unit(w, 1, 4 + k), (w.first, 4 + k), (w.second, k))
        for w in weights:
            third(w, k).start()

    received(s1_sem.at[2], like[6])
    received(s2_sem.at[0], like[6])
    each(0, 2, stage3)
    loaded(4, like[12])
    loaded(5, like[12])
    loaded(6, like[6])
    sent(all_send.at[0], like[24])
    tell(0, 0)
    received(s1_sem.at[3], like[6])
    sent(all_send.at[1], like[12])
    tell(1, 1)
    received(s2_sem.at[1], like[6])

    def update(k):
        for w in weights:
            third(w, k).wait()
            pl.semaphore_signal(third_free.at[w.i], inc=1, device_id={"dp": w.to[2]}, device_id_type=MESH)
            at = (k, *w.block(1, 1, 1))

            def body(rows, w=w, at=at):
                g = total(w, at, rows, (w.first, 6 + k), (w.second, 2 + k), (w.third, k)).astype(BF16).astype(F32)
                new, m, v = adamw(w.old[k, rows, :].astype(F32), w.m[k, rows, :], w.v[k, rows, :], g)
                w.m[k, rows, :] = m
                w.v[k, rows, :] = v
                w.all[(*at, core, rows, slice(None))] = new

            slabs(0, w.rows, body)

        for w in weights:
            pl.semaphore_wait(third_free.at[w.i], 1)
            gather3(w, k).start()

    each(0, 2, update)

    def own21(k):
        for w in weights:
            gather2(w, k).start()
        for w in weights:
            gather1(w, k, 0).start()

    told(1)
    told(0)
    each(0, 2, own21)

    pl.semaphore_signal(read_sem, inc=1, device_id={"dp": pair}, device_id_type=MESH)
    pl.semaphore_wait(read_sem, 1)

    def own0(k):
        for w in weights:
            gather0(w, 1, k).start()

    each(0, 2, own0)

    def back3(k):
        for w in weights:
            gather2(w, 2 + k).start()
        for w in weights:
            gather1(w, 2 + k, 1).start()
            gather0(w, 1, 2 + k).start()

    received(a3_sem, like[6])
    each(0, 2, back3)

    def back2(k):
        for w in weights:
            gather0(w, 1, k).start()

    received(a2_sem.at[0], like[6])
    for w in weights:
        gather1(w, 4, 2).start()
    for w in weights:
        gather1(w, 5, 3, 0, w.rows - w.part).start()
    for w in weights:
        gather1(w, 5, 4, w.rows - w.part, w.part).start()
    each(4, 6, back2)
    received(a2_sem.at[1], like[6])
    for w in weights:
        keep_late(w).start()
    each(6, 8, back2)

    def back1(k):
        for w in weights:
            gather0(w, 0, k).start()

    for n in (0, 1):
        received(a1_sem.at[n], like[6])
        each(2 * n, 2 * n + 2, back1)
    for w in weights:
        received(last_sem.at[w.i, 0], w.third.at[0])
        gather0(w, 0, 4).start()
    for w in weights:
        received(last_sem.at[w.i, 1], w.third.at[0, pl.ds(0, w.rows - w.part)])
        gather0(w, 0, 5, 0, w.rows - w.part).start()
    for w in weights:
        received(last_sem.at[w.i, 2], w.third.at[0, pl.ds(0, w.part)])
        gather0(w, 0, 5, w.rows - w.part, w.part).start()

    loaded(0, like[6])
    for n, units in ((2, 6), (3, 12), (4, 24)):
        sent(all_send.at[n], like[units])
    received(own_sem, like[24])
    for w in weights:
        sent(send_sem.at[w.i, 1], like[6])
    for w in weights:
        received(a0_sem.at[w.i], like[6])
        sent(send_sem.at[w.i, 2], like[6])


def put(*refs):
    sem = refs[-1]
    copies = [
        pltpu.make_async_copy(refs[i].at[k], refs[9 + i].at[k], sem.at[i, k]) for i in range(9) for k in range(LAYERS)
    ]
    for copy in copies:
        copy.start()
    for copy in copies:
        copy.wait()


def patch(which, *refs):
    n = len({i for i, _ in which})
    blocks, outs, sem = refs[n : n + len(which)], refs[n + len(which) : -1], refs[-1]
    index = {i: j for j, i in enumerate(sorted({i for i, _ in which}))}
    core = lax.axis_index("dp") % 2
    where = [(lax.axis_index("dp") // s) % 2 for s in STRIDES]
    copies = []
    for j, ((i, paired), block) in enumerate(zip(which, blocks, strict=True)):
        at = (slice(None), *Weight(ORDERS[i], where, core).block(0, 0, 0), 1 - core if paired else core)
        copies.append(pltpu.make_async_copy(block, outs[index[i]].at[at], sem.at[j]))
    for copy in copies:
        copy.start()
    for copy in copies:
        copy.wait()


def solution(mesh):
    def step(*arrays):
        shapes = [a.shape[1:] for a in arrays[6:9]]

        def cut(a, i):
            return a.reshape(LAYERS, 2, 2, 2, 2, *shapes[i])

        operands = [cut(a, n % 3) for n, a in enumerate(arrays[:6])] + list(arrays[6:])
        blocks = [(n, rows, columns) for n in (8, 4, 2, LAYERS) for rows, columns in shapes]
        outs = pl.pallas_call(
            kernel,
            out_shape=[pltpu.VMEM((LAYERS, 2, 2, 2, 2, *s), BF16) for s in shapes] + [pltpu.VMEM((LAYERS, *s), F32) for s in shapes] * 2 + [jax.ShapeDtypeStruct((LAYERS, *s), BF16) for s in shapes],
            in_specs=[pl.BlockSpec(memory_space=pl.ANY)] * 12,
            out_specs=[pl.BlockSpec(memory_space=pltpu.VMEM)] * 9 + [pl.BlockSpec(memory_space=pl.ANY)] * 3,
            scratch_shapes=[
                *(pltpu.VMEM(s, BF16) for s in blocks),
                *(pltpu.SemaphoreType.DMA(n) for n in ((7,), (3, 4), (), (4,), (2,), (3, 2), (), (2,), (2,), (3, 3), (), (3,), (5,), (3, 3), (3, 2))),
                *(pltpu.SemaphoreType.REGULAR(n) for n in ((2,), (3,), ())),
            ],
            compiler_params=pltpu.CompilerParams(collective_id=0, has_side_effects=True, vmem_limit_bytes=17 * 1024 * 1024),
            name="step",
        )(*operands)
        late = [lax.ppermute(o, "dp", [(d, d ^ STRIDES[order[0]]) for d in range(16)]) for o, order in zip(outs[9:], ORDERS, strict=True)]
        outs = [pltpu.with_memory_space_constraint(o, pltpu.VMEM) for o in outs[:9]]
        done = list(pl.pallas_call(
            put,
            out_shape=[jax.ShapeDtypeStruct(o.shape, o.dtype) for o in outs],
            in_specs=[pl.BlockSpec(memory_space=pl.ANY)] * 9,
            out_specs=[pl.BlockSpec(memory_space=pl.ANY)] * 9,
            scratch_shapes=[pltpu.SemaphoreType.DMA((9, LAYERS))],
            compiler_params=pltpu.CompilerParams(vmem_limit_bytes=17 * 1024 * 1024),
            cost_estimate=pl.CostEstimate(flops=PUT_FLOPS, bytes_accessed=2 * 43_000_000, transcendentals=0),
            name="put",
        )(*outs))
        for i in range(3):
            late[i], done[3 + i] = lax.optimization_barrier((late[i], done[3 + i]))
        theirs = [lax.ppermute(o, "dp", [(d, d ^ 1) for d in range(16)]) for o in late]
        came = {(i, paired): (theirs if paired else late)[i] for i in range(3) for paired in (0, 1)}
        for name, which in (("patch0", ((0, 0), (1, 0), (2, 0), (0, 1))), ("patch1", ((1, 1), (2, 1)))):
            of = sorted({i for i, _ in which})
            patched = pl.pallas_call(
                functools.partial(patch, which),
                out_shape=[jax.ShapeDtypeStruct(done[i].shape, BF16) for i in of],
                in_specs=[pl.BlockSpec(memory_space=pl.ANY)] * len(of) + [pl.BlockSpec(memory_space=pltpu.VMEM)] * len(which),
                out_specs=[pl.BlockSpec(memory_space=pl.ANY)] * len(of),
                input_output_aliases={j: j for j in range(len(of))},
                scratch_shapes=[pltpu.SemaphoreType.DMA((len(which),))],
                compiler_params=pltpu.CompilerParams(vmem_limit_bytes=17 * 1024 * 1024),
                name=name,
            )(*(done[i] for i in of), *(pltpu.with_memory_space_constraint(came[one], pltpu.VMEM) for one in which))
            for i, one in zip(of, patched, strict=True):
                done[i] = one
        whole = [o.reshape(a.shape) for o, a in zip(done[:3], arrays[3:6], strict=True)]
        return (*whole, *done[3:])

    all_of, part = P(None, None, None), P(None, "dp", None)
    return jax.shard_map(
        step,
        mesh=mesh,
        in_specs=(P(("rep", "dp"), None, None, None),) * 3 + (all_of,) * 3 + (part,) * 6,
        out_specs=(P("rep", None, None),) * 3 + (P("rep", "dp", None),) * 6,
        check_vma=False,
    )
```

```python
import functools

import jax
import jax.numpy as jnp
from jax import lax
from jax.experimental import pallas as pl
from jax.experimental.pallas import tpu as pltpu
from jax.sharding import PartitionSpec as P

BF16, F32 = jnp.bfloat16, jnp.float32
MESH = pl.DeviceIdType.MESH
LAYERS = 2
ORDERS = ((0, 1, 2), (1, 2, 0), (2, 0, 1))
STRIDES = (8, 4, 2)
SLAB = 16
EVERY = slice(None)
GRID = (LAYERS, 2, 2, 2, 2)
GRANT = 17 * 1024 * 1024
PARTS = (16, 16, 48)
PIECES = ((0, 0, 0, 1), (1, 0, 1, 2), (2, 1, 0, 2))
PUT_FLOPS = 200_000_000


def adamw(w, m, v, g):
    m = 0.9 * m + 0.1 * g
    v = 0.95 * v + 0.05 * g * g
    step = m * lax.rsqrt(v + 1e-8) + 0.1 * w
    return (w - 0.02 * step).astype(BF16), m, v


class Weight:
    def __init__(self, order, where, core, **refs):
        self.order, self.core = order, core
        self.mine = [where[axis] for axis in order]
        self.__dict__.update(refs)

    def place(self, *stages):
        xyz = [None] * 3
        for axis, coordinate in zip(self.order, stages, strict=True):
            xyz[axis] = coordinate
        return tuple(xyz)

    def own(self):
        return self.block(1, 1, 1)

    def far(self):
        return self.block(0, 0, 0)

    def block(self, keep1, keep2, keep3):
        return self.place(*(1 - m + k * (2 * m - 1) for m, k in zip(self.mine, (keep1, keep2, keep3), strict=True)))


def kernel(*refs):
    threes = (refs[i : i + 3] for i in range(0, 39, 3))
    g_refs, w_refs, m_refs, v_refs, all_refs, m_outs, v_outs, late_refs, mid_refs, firsts, seconds, thirds, olds = threes
    load_sem, pair_sem, rest_sem, s1_sem, s2_sem, s3_sem, a3_sem, a2_sem, a1_sem, last_sem, own_sem, a0_sem, all_send, send_sem, third_sem, free_sem, third_free, read_sem = refs[39:]

    me = lax.axis_index("dp")
    core = me % 2
    where = [(me // s) % 2 for s in STRIDES]
    partners = [me + s * (1 - 2 * b) for s, b in zip(STRIDES, where, strict=True)]
    pair = me + 1 - 2 * core

    weights = [
        Weight(
            ORDERS[i], where, core, i=i, part=PARTS[i], rows=olds[i].shape[1], g=g_refs[i], all=all_refs[i], m=m_outs[i], v=v_outs[i],
            first=firsts[i], second=seconds[i], third=thirds[i], old=olds[i], late=late_refs[i], mid=mid_refs[i],
            to=[partners[axis] for axis in ORDERS[i]],
        )
        for i in range(3)
    ]

    def remote(src, dst, send, recv, device):
        return pltpu.make_async_remote_copy(
            src_ref=src, dst_ref=dst, send_sem=send, recv_sem=recv, device_id={"dp": device}, device_id_type=MESH
        )

    gate = weights[0]
    like = {
        2: gate.third,
        6: gate.first.at[pl.ds(0, 6)],
        8: gate.first,
        12: gate.all.at[:, :, :, :, 0, pl.ds(0, 48)],
        16: gate.all.at[:, :, :, :, 0],
        24: gate.all.at[:, :, :, :, :, pl.ds(0, 48)],
    }

    def sent(sem, ref):
        remote(ref, ref, sem, own_sem, pair).wait_send()

    def received(sem, ref):
        remote(ref, ref, own_sem, sem, pair).wait_recv()

    def loaded(n, ref):
        pltpu.make_async_copy(ref, ref, load_sem.at[n]).wait()

    def unit(w, keep1, k):
        return (k % 2, *w.block(keep1, k // 4, (k // 2) % 2))

    def stage(w):
        return pltpu.make_async_copy(w.g.at[(EVERY, *w.far(), 1 - core)], w.old, load_sem.at[0])

    def load(w, n):
        m2, m3 = w.mine[1:]
        at = (EVERY, *w.place(1 - w.mine[0], *((1 - m2, 1 - m3), (1 - m2, m3), (m2, EVERY))[n]), core)
        return pltpu.make_async_copy(w.g.at[at], w.all.at[at], load_sem.at[(1, 2, 7)[n]])

    def load_rest(w):
        at = (EVERY, *w.place(w.mine[0], EVERY, EVERY), core)
        return pltpu.make_async_copy(w.g.at[at], w.all.at[at], load_sem.at[3])

    def load_m(w):
        return pltpu.make_async_copy(m_refs[w.i], w.m, load_sem.at[4])

    def load_v(w):
        return pltpu.make_async_copy(v_refs[w.i], w.v, load_sem.at[5])

    def load_w(w):
        return pltpu.make_async_copy(w_refs[w.i].at[(EVERY, *w.own(), core)], w.old, load_sem.at[6])

    def to_pair(w, keep1, k, recv=None):
        at, recv = unit(w, keep1, k), rest_sem if keep1 else pair_sem.at[w.i, recv]
        return remote(w.g.at[(*at, 1 - core)], w.all.at[(*at, core)], send_sem.at[w.i, 0], recv, pair)

    def staged_to_pair(w, k, lo, n, recv):
        rows = pl.ds(lo, n)
        return remote(
            w.old.at[k, rows], w.all.at[(*unit(w, 0, k), core, rows)], send_sem.at[w.i, 0], pair_sem.at[w.i, recv], pair
        )

    def first(w, k, lo=0, n=None):
        rows = pl.ds(lo, w.rows if n is None else n)
        at = (*unit(w, 0, k), core, rows)
        return remote(w.all.at[at], w.first.at[k, rows], all_send.at[0], s1_sem.at[k // 2], w.to[0])

    def second(w, k):
        at = (k % 2, *w.block(1, 0, k // 2))
        return remote(w.all.at[(*at, core)], w.second.at[k], all_send.at[1], s2_sem.at[k // 2], w.to[1])

    def third(w, k):
        at = (k, *w.block(1, 1, 0))
        return remote(w.all.at[(*at, core)], w.third.at[k], third_sem.at[w.i, k], s3_sem.at[w.i, k], w.to[2])

    def tell(n, stage):
        for w in weights:
            pl.semaphore_signal(free_sem.at[n], inc=1, device_id={"dp": w.to[stage]}, device_id_type=MESH)

    def told(n):
        pl.semaphore_wait(free_sem.at[n], 3)

    def gather3(w, k):
        at = (k, *w.own(), core)
        return remote(w.all.at[at], w.all.at[at], all_send.at[2], a3_sem, w.to[2])

    def gather2(w, k):
        at = (k % 2, *w.block(1, 1, 1 - k // 2), core)
        return remote(w.all.at[at], w.all.at[at], all_send.at[3], a2_sem.at[k // 2], w.to[1])

    def came(w, keep1, k, lo, n):
        return (k % 2, *w.block(keep1, 1 - k // 4, 1 - (k // 2) % 2), core, pl.ds(lo, w.rows if n is None else n))

    def gather1(w, k, recv, lo=0, n=None):
        at = came(w, 1, k, lo, n)
        sem = a1_sem.at[recv] if recv < 2 else last_sem.at[w.i, recv - 2]
        return remote(w.all.at[at], w.all.at[at], send_sem.at[w.i, 1], sem, w.to[0])

    def gather0(w, keep1, k, lo=0, n=None):
        at = came(w, keep1, k, lo, n)
        send, recv = (all_send.at[4], own_sem) if keep1 else (all_send.at[5], a0_sem)
        return remote(w.all.at[at], w.all.at[at], send, recv, pair)

    def keep_late(w):
        at = (EVERY, *w.block(1, 0, 0), core)
        return pltpu.make_async_copy(w.all.at[at], w.late, load_sem.at[0])

    def keep_mid(w, k, lo, n):
        rows = pl.ds(lo, n)
        return pltpu.make_async_copy(w.all.at[(k, *w.block(0, 0, 1), core, rows)], w.mid.at[k, rows], load_sem.at[1])

    def total(w, at, rows, *others):
        sum_ = w.all[(*at, core, rows, EVERY)].astype(F32) + w.all[(*at, 1 - core, rows, EVERY)].astype(F32)
        for other, k in others:
            sum_ = sum_ + other[k, rows, :].astype(F32)
        return sum_

    def slabs(lo, n, body):
        @pl.loop(0, n // SLAB)
        def _(r):
            body(pl.ds(pl.multiple_of(lo + r * SLAB, SLAB), SLAB))

    def add(w, at, *others, lo=0, n=None):
        def body(rows):
            w.all[(*at, core, rows, EVERY)] = total(w, at, rows, *others).astype(BF16)

        slabs(lo, w.rows if n is None else n, body)

    def each(lo, hi, body):
        @pl.loop(lo, hi)
        def _(k):
            body(k)

    for w in weights:
        stage(w).start()
    for w in weights:
        load(w, 0).start()

    barrier = pltpu.get_barrier_semaphore()
    for device in (pair, *partners):
        pl.semaphore_signal(barrier, inc=1, device_id={"dp": device}, device_id_type=MESH)
    loaded(0, like[6])
    pl.semaphore_wait(barrier, 4)

    for w in weights:
        staged_to_pair(w, 0, 0, w.part, 0).start()
    for w in weights:
        staged_to_pair(w, 0, w.part, w.rows - w.part, 1).start()
    for w in weights:
        staged_to_pair(w, 1, 0, w.rows, 2).start()

    def early(pieces, send):
        for recv, k, begin, end in pieces:
            for w in weights:
                edges = (0, w.part, w.rows)
                lo, n = edges[begin], edges[end] - edges[begin]
                received(pair_sem.at[w.i, recv], w.old.at[0, pl.ds(0, n)])
                add(w, unit(w, 0, k), lo=lo, n=n)
                if send:
                    first(w, k, lo, n).start()

    def start_pair(k, recv):
        for w in weights:
            to_pair(w, 0, k, recv).start()

    def start_pair_rest(k):
        for w in weights:
            to_pair(w, 1, k).start()

    def sum1(k):
        for w in weights:
            add(w, unit(w, 0, k))

    def send1(k):
        for w in weights:
            first(w, k).start()

    def stage1(k):
        sum1(k)
        send1(k)

    loaded(1, like[6])

    @pl.when(core == 0)
    def _():
        early(PIECES[:1], True)

    each(2, 4, lambda k: start_pair(k, 3))
    each(4, 8, lambda k: start_pair(k, 4))
    for n in (1, 2):
        for w in weights:
            load(w, n).start()

    @pl.when(core == 0)
    def _():
        early(PIECES[1:], True)

    each(0, 8, start_pair_rest)
    for w in weights:
        load_rest(w).start()
    loaded(2, like[6])

    @pl.when(core == 1)
    def _():
        early(PIECES, False)
        for w in weights:
            received(pair_sem.at[w.i, 3], w.old)
        each(2, 4, sum1)
        each(0, 4, send1)

    @pl.when(core == 0)
    def _():
        for w in weights:
            received(pair_sem.at[w.i, 3], w.old)
        each(2, 4, stage1)

    loaded(7, like[12])
    for w in weights:
        received(pair_sem.at[w.i, 4], w.second)
    each(4, 8, stage1)
    for w in weights:
        load_m(w).start()
        load_v(w).start()
    loaded(3, like[24])
    received(rest_sem, like[24])
    for w in weights:
        sent(send_sem.at[w.i, 0], like[16])
        load_w(w).start()

    def stage2(k):
        for w in weights:
            add(w, unit(w, 1, k), (w.first, k))
        for w in weights:
            second(w, k).start()

    for n in (0, 1):
        received(s1_sem.at[n], like[6])
        each(2 * n, 2 * n + 2, stage2)

    def stage3(k):
        for w in weights:
            add(w, unit(w, 1, 4 + k), (w.first, 4 + k), (w.second, k))
        for w in weights:
            third(w, k).start()

    received(s1_sem.at[2], like[6])
    received(s2_sem.at[0], like[6])
    each(0, 2, stage3)
    loaded(4, like[12])
    loaded(5, like[12])
    loaded(6, like[6])
    sent(all_send.at[0], like[24])
    tell(0, 0)
    received(s1_sem.at[3], like[6])
    sent(all_send.at[1], like[12])
    tell(1, 1)
    received(s2_sem.at[1], like[6])

    def update(k):
        for w in weights:
            third(w, k).wait()
            pl.semaphore_signal(third_free.at[w.i], inc=1, device_id={"dp": w.to[2]}, device_id_type=MESH)
            at = (k, *w.own())

            def body(rows, w=w, at=at):
                g = total(w, at, rows, (w.first, 6 + k), (w.second, 2 + k), (w.third, k)).astype(BF16).astype(F32)
                new, m, v = adamw(w.old[k, rows, :].astype(F32), w.m[k, rows, :], w.v[k, rows, :], g)
                w.m[k, rows, :] = m
                w.v[k, rows, :] = v
                w.all[(*at, core, rows, EVERY)] = new

            slabs(0, w.rows, body)

        for w in weights:
            pl.semaphore_wait(third_free.at[w.i], 1)
            gather3(w, k).start()

    each(0, 2, update)

    def own21(k):
        for w in weights:
            gather2(w, k).start()
        for w in weights:
            gather1(w, k, 0).start()

    told(1)
    told(0)
    each(0, 2, own21)

    pl.semaphore_signal(read_sem, inc=1, device_id={"dp": pair}, device_id_type=MESH)
    pl.semaphore_wait(read_sem, 1)

    def own0(k):
        for w in weights:
            gather0(w, 1, k).start()

    each(0, 2, own0)

    def back3(k):
        for w in weights:
            gather2(w, 2 + k).start()
        for w in weights:
            gather1(w, 2 + k, 1).start()
            gather0(w, 1, 2 + k).start()

    received(a3_sem, like[6])
    each(0, 2, back3)

    def back2(k):
        for w in weights:
            gather0(w, 1, k).start()

    received(a2_sem.at[0], like[6])
    for w in weights:
        gather1(w, 4, 2).start()
    for w in weights:
        gather1(w, 5, 3, 0, w.rows - w.part).start()
    for w in weights:
        gather1(w, 5, 4, w.rows - w.part, w.part).start()
    each(4, 6, back2)
    received(a2_sem.at[1], like[6])
    for w in weights:
        keep_late(w).start()
    each(6, 8, back2)

    def back1(k):
        for w in weights:
            gather0(w, 0, k).start()

    for n in (0, 1):
        received(a1_sem.at[n], like[6])
        each(2 * n, 2 * n + 2, back1)
    for w in weights:
        received(last_sem.at[w.i, 0], w.third.at[0])
        keep_mid(w, 0, 0, w.rows).start()
    for w in weights:
        received(last_sem.at[w.i, 1], w.third.at[0, pl.ds(0, w.rows - w.part)])
        keep_mid(w, 1, 0, w.rows - w.part).start()
    for w in weights:
        received(last_sem.at[w.i, 2], w.third.at[0, pl.ds(0, w.part)])
        keep_mid(w, 1, w.rows - w.part, w.part).start()

    loaded(0, like[6])
    for n, units in ((2, 6), (3, 12), (4, 24), (5, 12)):
        sent(all_send.at[n], like[units])
    received(own_sem, like[24])
    received(a0_sem, like[12])
    for w in weights:
        sent(send_sem.at[w.i, 1], like[6])
    loaded(1, like[6])


def blocks_of(i):
    me = lax.axis_index("dp")
    return Weight(ORDERS[i], [(me // s) % 2 for s in STRIDES], me % 2)


def run(copies):
    for copy in copies:
        copy.start()
    for copy in copies:
        copy.wait()


def put(*refs):
    ins, outs, sem = refs[:6], refs[6:12], refs[12]
    copies = []
    for i in range(3):
        w = blocks_of(i)
        here, every = w.own(), EVERY
        coordinates = [here[axis] for axis in w.order]
        for n, at in enumerate((
            (every, *w.place(coordinates[0], every, every)),
            (every, *w.place(1 - coordinates[0], coordinates[1], every)),
            (every, *w.block(0, 0, 1), w.core),
        )):
            copies.append(pltpu.make_async_copy(ins[i].at[at], outs[i].at[at], sem.at[i, n]))
        for k in range(LAYERS):
            copies.append(pltpu.make_async_copy(ins[3 + i].at[k], outs[3 + i].at[k], sem.at[3 + i, k]))
    run(copies)


def patch0(*refs):
    _, lates, mids, vs, outs, v_outs = (refs[i : i + 3] for i in range(0, 18, 3))
    sem = refs[-1]
    copies = []
    for i in range(3):
        w = blocks_of(i)
        copies.append(pltpu.make_async_copy(lates[i], outs[i].at[(EVERY, *w.far(), w.core)], sem.at[i, 0]))
        copies.append(pltpu.make_async_copy(mids[i], outs[i].at[(EVERY, *w.block(0, 0, 1), 1 - w.core)], sem.at[i, 1]))
        copies.append(pltpu.make_async_copy(vs[i], v_outs[i], sem.at[i, 2]))
    run(copies)


def patch1(*refs):
    theirs, outs, sem = refs[3:6], refs[6:9], refs[-1]
    copies = []
    for i in range(3):
        w = blocks_of(i)
        copies.append(pltpu.make_async_copy(theirs[i], outs[i].at[(EVERY, *w.far(), 1 - w.core)], sem.at[i]))
    run(copies)


def local(kernel_, name, outs, hbm, vmem, sems, cost=None):
    return list(
        pl.pallas_call(
            kernel_,
            out_shape=[jax.ShapeDtypeStruct(o.shape, o.dtype) for o in outs],
            in_specs=[pl.BlockSpec(memory_space=pl.ANY)] * len(hbm) + [pl.BlockSpec(memory_space=pltpu.VMEM)] * len(vmem),
            out_specs=[pl.BlockSpec(memory_space=pl.ANY)] * len(outs),
            input_output_aliases={j: j for j in range(len(hbm))},
            scratch_shapes=[pltpu.SemaphoreType.DMA(sems)],
            compiler_params=pltpu.CompilerParams(vmem_limit_bytes=GRANT),
            cost_estimate=cost,
            name=name,
        )(*hbm, *(pltpu.with_memory_space_constraint(o, pltpu.VMEM) for o in vmem))
    )


def solution(mesh):
    def step(*arrays):
        shapes = [a.shape[1:] for a in arrays[6:9]]

        def cut(a, i):
            return a.reshape(*GRID, *shapes[i])

        operands = [cut(a, n % 3) for n, a in enumerate(arrays[:6])] + list(arrays[6:])
        blocks = [(n, rows, columns) for n in (8, 4, 2, LAYERS) for rows, columns in shapes]
        outs = pl.pallas_call(
            kernel,
            out_shape=[pltpu.VMEM((*GRID, *s), BF16) for s in shapes] + [pltpu.VMEM((LAYERS, *s), F32) for s in shapes] * 2 + [jax.ShapeDtypeStruct((LAYERS, *s), BF16) for s in shapes] * 2,
            in_specs=[pl.BlockSpec(memory_space=pl.ANY)] * 12,
            out_specs=[pl.BlockSpec(memory_space=pltpu.VMEM)] * 9 + [pl.BlockSpec(memory_space=pl.ANY)] * 6,
            scratch_shapes=[
                *(pltpu.VMEM(s, BF16) for s in blocks),
                *(pltpu.SemaphoreType.DMA(n) for n in ((8,), (3, 5), (), (4,), (2,), (3, 2), (), (2,), (2,), (3, 3), (), (), (6,), (3, 2), (3, 2))),
                *(pltpu.SemaphoreType.REGULAR(n) for n in ((2,), (3,), ())),
            ],
            compiler_params=pltpu.CompilerParams(collective_id=0, has_side_effects=True, vmem_limit_bytes=GRANT),
            name="step",
        )(*operands)
        late = [lax.ppermute(o, "dp", [(d, d ^ STRIDES[order[0]]) for d in range(16)]) for o, order in zip(outs[9:12], ORDERS, strict=True)]
        over_pair = [(d, d ^ 1) for d in range(16)]
        mids = [lax.ppermute(o, "dp", over_pair) for o in outs[12:]]
        cost = pl.CostEstimate(flops=PUT_FLOPS, bytes_accessed=2 * 32_000_000, transcendentals=0)
        done = local(put, "put", outs[:6], [], outs[:6], (6, 3), cost)
        for i in range(3):
            late[i], done[3 + i] = lax.optimization_barrier((late[i], done[3 + i]))
        theirs = [lax.ppermute(o, "dp", over_pair) for o in late]
        some = local(patch0, "patch0", done[:3] + list(outs[6:9]), done[:3], [*late, *mids, *outs[6:9]], (3, 3))
        weights = local(patch1, "patch1", done[:3], some[:3], theirs, (3,))
        done = [*weights, *done[3:], *some[3:]]
        whole = [o.reshape(a.shape) for o, a in zip(done[:3], arrays[3:6], strict=True)]
        return (*whole, *done[3:])

    all_of, part = P(None, None, None), P(None, "dp", None)
    return jax.shard_map(
        step,
        mesh=mesh,
        in_specs=(P(("rep", "dp"), None, None, None),) * 3 + (all_of,) * 3 + (part,) * 6,
        out_specs=(P("rep", None, None),) * 3 + (P("rep", "dp", None),) * 6,
        check_vma=False,
    )
```

```python
import jax
import jax.numpy as jnp
from jax import lax
from jax.experimental import pallas as pl
from jax.experimental.pallas import tpu as pltpu
from jax.sharding import PartitionSpec as P


BF16, F32 = jnp.bfloat16, jnp.float32
MESH = pl.DeviceIdType.MESH
LAYERS = 2
ORDERS = ((0, 1, 2), (1, 2, 0), (2, 0, 1))
STRIDES = (8, 4, 2)
SLAB = 16
EVERY = slice(None)
GRID = (LAYERS, 2, 2, 2, 2)
GRANT = 17 * 1024 * 1024
PARTS = (16, 16, 48)
PIECES = ((0, 0, 0, 1), (1, 0, 1, 2), (2, 1, 0, 2))
PUT_FLOPS = 200_000_000


def adamw(w, m, v, g):
    m = 0.9 * m + 0.1 * g
    v = 0.95 * v + 0.05 * g * g
    step = m * lax.rsqrt(v + 1e-8) + 0.1 * w
    return (w - 0.02 * step).astype(BF16), m, v


class Weight:
    def __init__(self, order, where, core, **refs):
        self.order, self.core = order, core
        self.mine = [where[axis] for axis in order]
        self.__dict__.update(refs)

    def place(self, *stages):
        xyz = [None] * 3
        for axis, coordinate in zip(self.order, stages, strict=True):
            xyz[axis] = coordinate
        return tuple(xyz)

    def own(self):
        return self.block(1, 1, 1)

    def far(self):
        return self.block(0, 0, 0)

    def block(self, keep1, keep2, keep3):
        return self.place(*(1 - m + k * (2 * m - 1) for m, k in zip(self.mine, (keep1, keep2, keep3), strict=True)))


def kernel(*refs):
    threes = (refs[i : i + 3] for i in range(0, 39, 3))
    g_refs, w_refs, m_refs, v_refs, all_refs, m_outs, v_outs, late_refs, mid_refs, firsts, seconds, thirds, olds = threes
    load_sem, pair_sem, rest_sem, s1_sem, s2_sem, s3_sem, a3_sem, a2_sem, a1_sem, last_sem, own_sem, a0_sem, all_send, send_sem, third_sem, free_sem, third_free, read_sem = refs[39:]

    me = lax.axis_index("dp")
    core = me % 2
    where = [(me // s) % 2 for s in STRIDES]
    partners = [me + s * (1 - 2 * b) for s, b in zip(STRIDES, where, strict=True)]
    pair = me + 1 - 2 * core

    weights = [
        Weight(
            ORDERS[i], where, core, i=i, part=PARTS[i], rows=olds[i].shape[1], g=g_refs[i], all=all_refs[i], m=m_outs[i], v=v_outs[i],
            first=firsts[i], second=seconds[i], third=thirds[i], old=olds[i], late=late_refs[i], mid=mid_refs[i],
            to=[partners[axis] for axis in ORDERS[i]],
        )
        for i in range(3)
    ]

    def remote(src, dst, send, recv, device):
        return pltpu.make_async_remote_copy(
            src_ref=src, dst_ref=dst, send_sem=send, recv_sem=recv, device_id={"dp": device}, device_id_type=MESH
        )

    gate = weights[0]
    like = {
        2: gate.third,
        6: gate.first.at[pl.ds(0, 6)],
        8: gate.first,
        12: gate.all.at[:, :, :, :, 0, pl.ds(0, 48)],
        16: gate.all.at[:, :, :, :, 0],
        24: gate.all.at[:, :, :, :, :, pl.ds(0, 48)],
    }

    def sent(sem, ref):
        remote(ref, ref, sem, own_sem, pair).wait_send()

    def received(sem, ref):
        remote(ref, ref, own_sem, sem, pair).wait_recv()

    def loaded(n, ref):
        pltpu.make_async_copy(ref, ref, load_sem.at[n]).wait()

    def unit(w, keep1, k):
        return (k % 2, *w.block(keep1, k // 4, (k // 2) % 2))

    def stage(w):
        return pltpu.make_async_copy(w.g.at[(EVERY, *w.far(), 1 - core)], w.old, load_sem.at[0])

    def load(w, n):
        m2, m3 = w.mine[1:]
        at = (EVERY, *w.place(1 - w.mine[0], *((1 - m2, 1 - m3), (1 - m2, m3), (m2, EVERY))[n]), core)
        return pltpu.make_async_copy(w.g.at[at], w.all.at[at], load_sem.at[(1, 2, 7)[n]])

    def load_rest(w):
        at = (EVERY, *w.place(w.mine[0], EVERY, EVERY), core)
        return pltpu.make_async_copy(w.g.at[at], w.all.at[at], load_sem.at[3])

    def load_m(w):
        return pltpu.make_async_copy(m_refs[w.i], w.m, load_sem.at[4])

    def load_v(w):
        return pltpu.make_async_copy(v_refs[w.i], w.v, load_sem.at[5])

    def load_w(w):
        return pltpu.make_async_copy(w_refs[w.i].at[(EVERY, *w.own(), core)], w.old, load_sem.at[6])

    def to_pair(w, keep1, k, recv=None):
        at, recv = unit(w, keep1, k), rest_sem if keep1 else pair_sem.at[w.i, recv]
        return remote(w.g.at[(*at, 1 - core)], w.all.at[(*at, core)], send_sem.at[w.i, 0], recv, pair)

    def staged_to_pair(w, k, lo, n, recv):
        rows = pl.ds(lo, n)
        return remote(
            w.old.at[k, rows], w.all.at[(*unit(w, 0, k), core, rows)], send_sem.at[w.i, 0], pair_sem.at[w.i, recv], pair
        )

    def first(w, k, lo=0, n=None):
        rows = pl.ds(lo, w.rows if n is None else n)
        at = (*unit(w, 0, k), core, rows)
        return remote(w.all.at[at], w.first.at[k, rows], all_send.at[0], s1_sem.at[k // 2], w.to[0])

    def second(w, k):
        at = (k % 2, *w.block(1, 0, k // 2))
        return remote(w.all.at[(*at, core)], w.second.at[k], all_send.at[1], s2_sem.at[k // 2], w.to[1])

    def third(w, k):
        at = (k, *w.block(1, 1, 0))
        return remote(w.all.at[(*at, core)], w.third.at[k], third_sem.at[w.i, k], s3_sem.at[w.i, k], w.to[2])

    def tell(n, stage):
        for w in weights:
            pl.semaphore_signal(free_sem.at[n], inc=1, device_id={"dp": w.to[stage]}, device_id_type=MESH)

    def told(n):
        pl.semaphore_wait(free_sem.at[n], 3)

    def gather3(w, k):
        at = (k, *w.own(), core)
        return remote(w.all.at[at], w.all.at[at], all_send.at[2], a3_sem, w.to[2])

    def gather2(w, k):
        at = (k % 2, *w.block(1, 1, 1 - k // 2), core)
        return remote(w.all.at[at], w.all.at[at], all_send.at[3], a2_sem.at[k // 2], w.to[1])

    def came(w, keep1, k, lo, n):
        return (k % 2, *w.block(keep1, 1 - k // 4, 1 - (k // 2) % 2), core, pl.ds(lo, w.rows if n is None else n))

    def gather1(w, k, recv, lo=0, n=None):
        at = came(w, 1, k, lo, n)
        sem = a1_sem.at[recv] if recv < 2 else last_sem.at[w.i, recv - 2]
        return remote(w.all.at[at], w.all.at[at], send_sem.at[w.i, 1], sem, w.to[0])

    def gather0(w, keep1, k, lo=0, n=None):
        at = came(w, keep1, k, lo, n)
        send, recv = (all_send.at[4], own_sem) if keep1 else (all_send.at[5], a0_sem)
        return remote(w.all.at[at], w.all.at[at], send, recv, pair)

    def keep_late(w):
        at = (EVERY, *w.block(1, 0, 0), core)
        return pltpu.make_async_copy(w.all.at[at], w.late, load_sem.at[0])

    def keep_mid(w, k, lo, n):
        rows = pl.ds(lo, n)
        return pltpu.make_async_copy(w.all.at[(k, *w.block(0, 0, 1), core, rows)], w.mid.at[k, rows], load_sem.at[1])

    def total(w, at, rows, *others):
        sum_ = w.all[(*at, core, rows, EVERY)].astype(F32) + w.all[(*at, 1 - core, rows, EVERY)].astype(F32)
        for other, k in others:
            sum_ = sum_ + other[k, rows, :].astype(F32)
        return sum_

    def slabs(lo, n, body):
        @pl.loop(0, n // SLAB)
        def _(r):
            body(pl.ds(pl.multiple_of(lo + r * SLAB, SLAB), SLAB))

    def add(w, at, *others, lo=0, n=None):
        def body(rows):
            w.all[(*at, core, rows, EVERY)] = total(w, at, rows, *others).astype(BF16)

        slabs(lo, w.rows if n is None else n, body)

    def each(lo, hi, body):
        @pl.loop(lo, hi)
        def _(k):
            body(k)

    for w in weights:
        stage(w).start()
    for w in weights:
        load(w, 0).start()

    barrier = pltpu.get_barrier_semaphore()
    for device in (pair, *partners):
        pl.semaphore_signal(barrier, inc=1, device_id={"dp": device}, device_id_type=MESH)
    loaded(0, like[6])
    pl.semaphore_wait(barrier, 4)

    for w in weights:
        staged_to_pair(w, 0, 0, w.part, 0).start()
    for w in weights:
        staged_to_pair(w, 0, w.part, w.rows - w.part, 1).start()
    for w in weights:
        staged_to_pair(w, 1, 0, w.rows, 2).start()

    def early(pieces, send):
        for recv, k, begin, end in pieces:
            for w in weights:
                edges = (0, w.part, w.rows)
                lo, n = edges[begin], edges[end] - edges[begin]
                received(pair_sem.at[w.i, recv], w.old.at[0, pl.ds(0, n)])
                add(w, unit(w, 0, k), lo=lo, n=n)
                if send:
                    first(w, k, lo, n).start()

    def start_pair(k, recv):
        for w in weights:
            to_pair(w, 0, k, recv).start()

    def start_pair_rest(k):
        for w in weights:
            to_pair(w, 1, k).start()

    def sum1(k):
        for w in weights:
            add(w, unit(w, 0, k))

    def send1(k):
        for w in weights:
            first(w, k).start()

    def stage1(k):
        sum1(k)
        send1(k)

    loaded(1, like[6])

    @pl.when(core == 0)
    def _():
        early(PIECES[:1], True)

    each(2, 4, lambda k: start_pair(k, 3))
    each(4, 8, lambda k: start_pair(k, 4))
    for n in (1, 2):
        for w in weights:
            load(w, n).start()

    @pl.when(core == 0)
    def _():
        early(PIECES[1:], True)

    each(0, 8, start_pair_rest)
    for w in weights:
        load_rest(w).start()
    loaded(2, like[6])

    @pl.when(core == 1)
    def _():
        early(PIECES, False)
        for w in weights:
            received(pair_sem.at[w.i, 3], w.old)
        each(2, 4, sum1)
        each(0, 4, send1)

    @pl.when(core == 0)
    def _():
        for w in weights:
            received(pair_sem.at[w.i, 3], w.old)
        each(2, 4, stage1)

    loaded(7, like[12])
    for w in weights:
        received(pair_sem.at[w.i, 4], w.second)
    each(4, 8, stage1)
    for w in weights:
        load_m(w).start()
        load_v(w).start()
    loaded(3, like[24])
    received(rest_sem, like[24])
    for w in weights:
        sent(send_sem.at[w.i, 0], like[16])
        load_w(w).start()

    def stage2(k):
        for w in weights:
            add(w, unit(w, 1, k), (w.first, k))
        for w in weights:
            second(w, k).start()

    for n in (0, 1):
        received(s1_sem.at[n], like[6])
        each(2 * n, 2 * n + 2, stage2)

    def stage3(k):
        for w in weights:
            add(w, unit(w, 1, 4 + k), (w.first, 4 + k), (w.second, k))
        for w in weights:
            third(w, k).start()

    received(s1_sem.at[2], like[6])
    received(s2_sem.at[0], like[6])
    each(0, 2, stage3)
    loaded(4, like[12])
    loaded(5, like[12])
    loaded(6, like[6])
    sent(all_send.at[0], like[24])
    tell(0, 0)
    received(s1_sem.at[3], like[6])
    sent(all_send.at[1], like[12])
    tell(1, 1)
    received(s2_sem.at[1], like[6])

    def update(k):
        for w in weights:
            third(w, k).wait()
            pl.semaphore_signal(third_free.at[w.i], inc=1, device_id={"dp": w.to[2]}, device_id_type=MESH)
            at = (k, *w.own())

            def body(rows, w=w, at=at):
                g = total(w, at, rows, (w.first, 6 + k), (w.second, 2 + k), (w.third, k)).astype(BF16).astype(F32)
                new, m, v = adamw(w.old[k, rows, :].astype(F32), w.m[k, rows, :], w.v[k, rows, :], g)
                w.m[k, rows, :] = m
                w.v[k, rows, :] = v
                w.all[(*at, core, rows, EVERY)] = new

            slabs(0, w.rows, body)

        for w in weights:
            pl.semaphore_wait(third_free.at[w.i], 1)
            gather3(w, k).start()

    each(0, 2, update)

    def own21(k):
        for w in weights:
            gather2(w, k).start()
        for w in weights:
            gather1(w, k, 0).start()

    told(1)
    told(0)
    each(0, 2, own21)

    pl.semaphore_signal(read_sem, inc=1, device_id={"dp": pair}, device_id_type=MESH)
    pl.semaphore_wait(read_sem, 1)

    def own0(k):
        for w in weights:
            gather0(w, 1, k).start()

    each(0, 2, own0)

    def back3(k):
        for w in weights:
            gather2(w, 2 + k).start()
        for w in weights:
            gather1(w, 2 + k, 1).start()
            gather0(w, 1, 2 + k).start()

    received(a3_sem, like[6])
    each(0, 2, back3)

    def back2(k):
        for w in weights:
            gather0(w, 1, k).start()

    received(a2_sem.at[0], like[6])
    for w in weights:
        gather1(w, 4, 2).start()
    for w in weights:
        gather1(w, 5, 3, 0, w.rows - w.part).start()
    for w in weights:
        gather1(w, 5, 4, w.rows - w.part, w.part).start()
    each(4, 6, back2)
    received(a2_sem.at[1], like[6])
    for w in weights:
        keep_late(w).start()
    each(6, 8, back2)

    def back1(k):
        for w in weights:
            gather0(w, 0, k).start()

    for n in (0, 1):
        received(a1_sem.at[n], like[6])
        each(2 * n, 2 * n + 2, back1)
    for w in weights:
        received(last_sem.at[w.i, 0], w.third.at[0])
        keep_mid(w, 0, 0, w.rows).start()
    for w in weights:
        received(last_sem.at[w.i, 1], w.third.at[0, pl.ds(0, w.rows - w.part)])
        keep_mid(w, 1, 0, w.rows - w.part).start()
    for w in weights:
        received(last_sem.at[w.i, 2], w.third.at[0, pl.ds(0, w.part)])
        keep_mid(w, 1, w.rows - w.part, w.part).start()

    loaded(0, like[6])
    for n, units in ((2, 6), (3, 12), (4, 24), (5, 12)):
        sent(all_send.at[n], like[units])
    received(own_sem, like[24])
    received(a0_sem, like[12])
    for w in weights:
        sent(send_sem.at[w.i, 1], like[6])
    loaded(1, like[6])


def blocks_of(i):
    me = lax.axis_index("dp")
    return Weight(ORDERS[i], [(me // s) % 2 for s in STRIDES], me % 2)


def run(copies):
    for copy in copies:
        copy.start()
    for copy in copies:
        copy.wait()


def put(*refs):
    ins, outs, sem = refs[:6], refs[6:12], refs[12]
    copies = []
    for i in range(3):
        w = blocks_of(i)
        here, every = w.own(), EVERY
        coordinates = [here[axis] for axis in w.order]
        for n, at in enumerate((
            (every, *w.place(coordinates[0], every, every)),
            (every, *w.place(1 - coordinates[0], coordinates[1], every)),
            (every, *w.block(0, 0, 1), w.core),
        )):
            copies.append(pltpu.make_async_copy(ins[i].at[at], outs[i].at[at], sem.at[i, n]))
        for k in range(LAYERS):
            copies.append(pltpu.make_async_copy(ins[3 + i].at[k], outs[3 + i].at[k], sem.at[3 + i, k]))
    run(copies)


def patch_mid(*refs):
    mids, outs, sem = refs[3:6], refs[6:9], refs[-1]
    copies = []
    for i in range(3):
        w = blocks_of(i)
        copies.append(pltpu.make_async_copy(mids[i], outs[i].at[(EVERY, *w.block(0, 0, 1), 1 - w.core)], sem.at[i]))
    run(copies)


def patch0(*refs):
    _, lates, vs, outs, v_outs = (refs[i : i + 3] for i in range(0, 15, 3))
    sem = refs[-1]
    copies = []
    for i in range(3):
        w = blocks_of(i)
        copies.append(pltpu.make_async_copy(lates[i], outs[i].at[(EVERY, *w.far(), w.core)], sem.at[i, 0]))
        copies.append(pltpu.make_async_copy(vs[i], v_outs[i], sem.at[i, 1]))
    run(copies)


def patch1(*refs):
    theirs, outs, sem = refs[3:6], refs[6:9], refs[-1]
    copies = []
    for i in range(3):
        w = blocks_of(i)
        copies.append(pltpu.make_async_copy(theirs[i], outs[i].at[(EVERY, *w.far(), 1 - w.core)], sem.at[i]))
    run(copies)


def local(kernel_, outs, hbm, vmem, sems, cost=None):
    return list(
        pl.pallas_call(
            kernel_,
            out_shape=[jax.ShapeDtypeStruct(o.shape, o.dtype) for o in outs],
            in_specs=[pl.BlockSpec(memory_space=pl.ANY)] * len(hbm) + [pl.BlockSpec(memory_space=pltpu.VMEM)] * len(vmem),
            out_specs=[pl.BlockSpec(memory_space=pl.ANY)] * len(outs),
            input_output_aliases={j: j for j in range(len(hbm))},
            scratch_shapes=[pltpu.SemaphoreType.DMA(sems)],
            compiler_params=pltpu.CompilerParams(vmem_limit_bytes=GRANT),
            cost_estimate=cost,
        )(*hbm, *(pltpu.with_memory_space_constraint(o, pltpu.VMEM) for o in vmem))
    )


def solution(mesh):
    def whole_step(*arrays):
        shapes = [a.shape[1:] for a in arrays[6:9]]

        def cut(a, i):
            return a.reshape(*GRID, *shapes[i])

        operands = [cut(a, n % 3) for n, a in enumerate(arrays[:6])] + list(arrays[6:])
        blocks = [(n, rows, columns) for n in (8, 4, 2, LAYERS) for rows, columns in shapes]
        outs = pl.pallas_call(
            kernel,
            out_shape=[pltpu.VMEM((*GRID, *s), BF16) for s in shapes] + [pltpu.VMEM((LAYERS, *s), F32) for s in shapes] * 2 + [jax.ShapeDtypeStruct((LAYERS, *s), BF16) for s in shapes] * 2,
            in_specs=[pl.BlockSpec(memory_space=pl.ANY)] * 12,
            out_specs=[pl.BlockSpec(memory_space=pltpu.VMEM)] * 9 + [pl.BlockSpec(memory_space=pl.ANY)] * 6,
            scratch_shapes=[
                *(pltpu.VMEM(s, BF16) for s in blocks),
                *(pltpu.SemaphoreType.DMA(n) for n in ((8,), (3, 5), (), (4,), (2,), (3, 2), (), (2,), (2,), (3, 3), (), (), (6,), (3, 2), (3, 2))),
                *(pltpu.SemaphoreType.REGULAR(n) for n in ((2,), (3,), ())),
            ],
            compiler_params=pltpu.CompilerParams(collective_id=0, has_side_effects=True, vmem_limit_bytes=GRANT),
            name="step",
        )(*operands)

        def axis(i):
            return lax.ppermute(outs[9 + i], "dp", [(d, d ^ STRIDES[ORDERS[i][0]]) for d in range(16)])

        def over(o):
            return lax.ppermute(o, "dp", [(d, d ^ 1) for d in range(16)])

        late = [axis(i) for i in range(3)]
        mids = [over(o) for o in outs[12:]]
        cost = pl.CostEstimate(flops=PUT_FLOPS, bytes_accessed=2 * 32_000_000, transcendentals=0)
        done = local(put, outs[:6], [], outs[:6], (6, 3), cost)
        for i in range(3):
            late[i], done[3 + i] = lax.optimization_barrier((late[i], done[3 + i]))
        theirs = [over(late[i]) for i in range(2)]
        some = local(patch_mid, done[:3], done[:3], mids, (3,))
        late[2], some[0] = lax.optimization_barrier((late[2], some[0]))
        theirs.append(over(late[2]))
        some = local(patch0, some + list(outs[6:9]), some, [*late, *outs[6:9]], (3, 2))
        weights = local(patch1, done[:3], some[:3], theirs, (3,))
        done = [*weights, *done[3:], *some[3:]]
        whole = [o.reshape(a.shape) for o, a in zip(done[:3], arrays[3:6], strict=True)]
        return (*whole, *done[3:])

    all_of, part = P(None, None, None), P(None, "dp", None)
    return jax.shard_map(
        whole_step,
        mesh=mesh,
        in_specs=(P(("rep", "dp"), None, None, None),) * 3 + (all_of,) * 3 + (part,) * 6,
        out_specs=(P("rep", None, None),) * 3 + (P("rep", "dp", None),) * 6,
        check_vma=False,
    )
```

```python
import jax
import jax.numpy as jnp
from jax import lax
from jax.experimental import pallas as pl
from jax.experimental.pallas import tpu as pltpu
from jax.sharding import PartitionSpec as P


BF16, F32 = jnp.bfloat16, jnp.float32
MESH = pl.DeviceIdType.MESH
LAYERS = 2
ORDERS = ((0, 1, 2), (1, 2, 0), (2, 0, 1))
STRIDES = (8, 4, 2)
SLAB = 16
EARLY = 7
EVERY = slice(None)
GRID = (LAYERS, 2, 2, 2, 2)
GRANT = 17 * 1024 * 1024
PARTS = (16, 16, 48)
PIECES = ((0, 0, 0, 1), (1, 0, 1, 2), (2, 1, 0, 2))
PUT_FLOPS = 200_000_000


def adamw(w, m, v, g):
    m = 0.9 * m + 0.1 * g
    v = 0.95 * v + 0.05 * g * g
    step = m * lax.rsqrt(v + 1e-8) + 0.1 * w
    return (w - 0.02 * step).astype(BF16), m, v


class Weight:
    def __init__(self, order, where, core, **refs):
        self.order, self.core = order, core
        self.mine = [where[axis] for axis in order]
        self.__dict__.update(refs)

    def place(self, *stages):
        xyz = [None] * 3
        for axis, coordinate in zip(self.order, stages, strict=True):
            xyz[axis] = coordinate
        return tuple(xyz)

    def own(self):
        return self.block(1, 1, 1)

    def far(self):
        return self.block(0, 0, 0)

    def block(self, keep1, keep2, keep3):
        return self.place(*(1 - m + k * (2 * m - 1) for m, k in zip(self.mine, (keep1, keep2, keep3), strict=True)))


def kernel(*refs):
    threes = (refs[i : i + 3] for i in range(0, 39, 3))
    g_refs, w_refs, m_refs, v_refs, all_refs, m_outs, v_outs, late_refs, mid_refs, firsts, seconds, thirds, olds = threes
    load_sem, pair_sem, rest_sem, s1_sem, s2_sem, s3_sem, a3_sem, a2_sem, a1_sem, last_sem, own_sem, a0_sem, all_send, send_sem, third_sem, free_sem, third_free, read_sem = refs[39:]

    me = lax.axis_index("dp")
    core = me % 2
    where = [(me // s) % 2 for s in STRIDES]
    partners = [me + s * (1 - 2 * b) for s, b in zip(STRIDES, where, strict=True)]
    pair = me + 1 - 2 * core

    weights = [
        Weight(
            ORDERS[i], where, core, i=i, part=PARTS[i], rows=olds[i].shape[1], g=g_refs[i], all=all_refs[i], m=m_outs[i], v=v_outs[i],
            first=firsts[i], second=seconds[i], third=thirds[i], old=olds[i], late=late_refs[i], mid=mid_refs[i],
            to=[partners[axis] for axis in ORDERS[i]],
        )
        for i in range(3)
    ]

    def remote(src, dst, send, recv, device):
        return pltpu.make_async_remote_copy(
            src_ref=src, dst_ref=dst, send_sem=send, recv_sem=recv, device_id={"dp": device}, device_id_type=MESH
        )

    gate = weights[0]
    like = {
        2: gate.third,
        6: gate.first.at[pl.ds(0, 6)],
        8: gate.first,
        12: gate.all.at[:, :, :, :, 0, pl.ds(0, 48)],
        16: gate.all.at[:, :, :, :, 0],
        24: gate.all.at[:, :, :, :, :, pl.ds(0, 48)],
    }

    def sent(sem, ref):
        remote(ref, ref, sem, own_sem, pair).wait_send()

    def received(sem, ref):
        remote(ref, ref, own_sem, sem, pair).wait_recv()

    def loaded(n, ref):
        pltpu.make_async_copy(ref, ref, load_sem.at[n]).wait()

    def unit(w, keep1, k):
        return (k % 2, *w.block(keep1, k // 4, (k // 2) % 2))

    def stage(w):
        return pltpu.make_async_copy(w.g.at[(EVERY, *w.far(), 1 - core)], w.old, load_sem.at[0])

    def load(w, n):
        m2, m3 = w.mine[1:]
        at = (EVERY, *w.place(1 - w.mine[0], *((1 - m2, 1 - m3), (1 - m2, m3), (m2, EVERY))[n]), core)
        return pltpu.make_async_copy(w.g.at[at], w.all.at[at], load_sem.at[(1, 2, 7)[n]])

    def load_rest(w):
        at = (EVERY, *w.place(w.mine[0], EVERY, EVERY), core)
        return pltpu.make_async_copy(w.g.at[at], w.all.at[at], load_sem.at[3])

    def load_m(w):
        return pltpu.make_async_copy(m_refs[w.i], w.m, load_sem.at[4])

    def load_v(w):
        return pltpu.make_async_copy(v_refs[w.i], w.v, load_sem.at[5])

    def load_w(w):
        return pltpu.make_async_copy(w_refs[w.i].at[(EVERY, *w.own(), core)], w.old, load_sem.at[6])

    def to_pair(w, keep1, k, recv=None):
        at, recv = unit(w, keep1, k), rest_sem if keep1 else pair_sem.at[w.i, recv]
        return remote(w.g.at[(*at, 1 - core)], w.all.at[(*at, core)], send_sem.at[w.i, 0], recv, pair)

    def staged_to_pair(w, k, lo, n, recv):
        rows = pl.ds(lo, n)
        return remote(
            w.old.at[k, rows], w.all.at[(*unit(w, 0, k), core, rows)], send_sem.at[w.i, 0], pair_sem.at[w.i, recv], pair
        )

    def first(w, k, lo=0, n=None):
        rows = pl.ds(lo, w.rows if n is None else n)
        at = (*unit(w, 0, k), core, rows)
        return remote(w.all.at[at], w.first.at[k, rows], all_send.at[0], s1_sem.at[k // 2], w.to[0])

    def second(w, k):
        at = (k % 2, *w.block(1, 0, k // 2))
        return remote(w.all.at[(*at, core)], w.second.at[k], all_send.at[1], s2_sem.at[k // 2], w.to[1])

    def third(w, k):
        at = (k, *w.block(1, 1, 0))
        return remote(w.all.at[(*at, core)], w.third.at[k], third_sem.at[w.i, k], s3_sem.at[w.i, k], w.to[2])

    def tell(n, stage):
        for w in weights:
            pl.semaphore_signal(free_sem.at[n], inc=1, device_id={"dp": w.to[stage]}, device_id_type=MESH)

    def told(n):
        pl.semaphore_wait(free_sem.at[n], 3)

    def gather3(w, k):
        at = (k, *w.own(), core)
        return remote(w.all.at[at], w.all.at[at], all_send.at[2], a3_sem, w.to[2])

    def gather2(w, k):
        at = (k % 2, *w.block(1, 1, 1 - k // 2), core)
        return remote(w.all.at[at], w.all.at[at], all_send.at[3], a2_sem.at[k // 2], w.to[1])

    def came(w, keep1, k, lo, n):
        return (k % 2, *w.block(keep1, 1 - k // 4, 1 - (k // 2) % 2), core, pl.ds(lo, w.rows if n is None else n))

    def gather1(w, k, recv, lo=0, n=None):
        at = came(w, 1, k, lo, n)
        sem = a1_sem.at[recv] if recv < 2 else last_sem.at[w.i, recv - 2]
        return remote(w.all.at[at], w.all.at[at], send_sem.at[w.i, 1], sem, w.to[0])

    def gather0(w, keep1, k, lo=0, n=None):
        at = came(w, keep1, k, lo, n)
        send, recv = (all_send.at[4], own_sem) if keep1 else (all_send.at[5], a0_sem)
        return remote(w.all.at[at], w.all.at[at], send, recv, pair)

    def keep_late(w):
        at = (EVERY, *w.block(1, 0, 0), core)
        return pltpu.make_async_copy(w.all.at[at], w.late, load_sem.at[0])

    def keep_mid(w, k, lo, n):
        rows = pl.ds(lo, n)
        return pltpu.make_async_copy(w.all.at[(k, *w.block(0, 0, 1), core, rows)], w.mid.at[k, rows], load_sem.at[1])

    def total(w, at, rows, *others):
        sum_ = w.all[(*at, core, rows, EVERY)].astype(F32) + w.all[(*at, 1 - core, rows, EVERY)].astype(F32)
        for other, k in others:
            sum_ = sum_ + other[k, rows, :].astype(F32)
        return sum_

    def slabs(lo, n, body):
        @pl.loop(0, n // SLAB)
        def _(r):
            body(pl.ds(pl.multiple_of(lo + r * SLAB, SLAB), SLAB))

    def add(w, at, *others, lo=0, n=None):
        def body(rows):
            w.all[(*at, core, rows, EVERY)] = total(w, at, rows, *others).astype(BF16)

        slabs(lo, w.rows if n is None else n, body)

    def each(lo, hi, body):
        @pl.loop(lo, hi)
        def _(k):
            body(k)

    for w in weights:
        stage(w).start()
    for w in weights:
        load(w, 0).start()

    barrier = pltpu.get_barrier_semaphore()
    for device in (pair, *partners):
        pl.semaphore_signal(barrier, inc=1, device_id={"dp": device}, device_id_type=MESH)
    loaded(0, like[6])
    pl.semaphore_wait(barrier, 4)

    for w in weights:
        staged_to_pair(w, 0, 0, w.part, 0).start()
    for w in weights:
        staged_to_pair(w, 0, w.part, w.rows - w.part, 1).start()
    for w in weights:
        staged_to_pair(w, 1, 0, w.rows, 2).start()

    def early(pieces, send):
        for recv, k, begin, end in pieces:
            for w in weights:
                edges = (0, w.part, w.rows)
                lo, n = edges[begin], edges[end] - edges[begin]
                received(pair_sem.at[w.i, recv], w.old.at[0, pl.ds(0, n)])
                add(w, unit(w, 0, k), lo=lo, n=n)
                if send:
                    first(w, k, lo, n).start()

    def start_pair(k, recv):
        for w in weights:
            to_pair(w, 0, k, recv).start()

    def start_pair_rest(k):
        for w in weights:
            to_pair(w, 1, k).start()

    def sum1(k):
        for w in weights:
            add(w, unit(w, 0, k))

    def send1(k):
        for w in weights:
            first(w, k).start()

    def stage1(k):
        sum1(k)
        send1(k)

    loaded(1, like[6])

    @pl.when(core == 0)
    def _():
        early(PIECES[:1], True)

    each(2, 4, lambda k: start_pair(k, 3))
    each(4, 8, lambda k: start_pair(k, 4))
    for n in (1, 2):
        for w in weights:
            load(w, n).start()

    @pl.when(core == 0)
    def _():
        early(PIECES[1:], True)

    each(0, 8, start_pair_rest)
    for w in weights:
        load_rest(w).start()
    loaded(2, like[6])

    @pl.when(core == 1)
    def _():
        early(PIECES, False)
        for w in weights:
            received(pair_sem.at[w.i, 3], w.old)
        each(2, 4, sum1)
        each(0, 4, send1)

    @pl.when(core == 0)
    def _():
        for w in weights:
            received(pair_sem.at[w.i, 3], w.old)
        each(2, 4, stage1)

    loaded(7, like[12])
    for w in weights:
        received(pair_sem.at[w.i, 4], w.second)
    each(4, 8, stage1)
    for w in weights:
        load_m(w).start()
        load_v(w).start()
    loaded(3, like[24])
    received(rest_sem, like[24])
    for w in weights:
        sent(send_sem.at[w.i, 0], like[16])
        load_w(w).start()

    def stage2(k):
        for w in weights:
            add(w, unit(w, 1, k), (w.first, k))
        for w in weights:
            second(w, k).start()

    for n in (0, 1):
        received(s1_sem.at[n], like[6])
        each(2 * n, 2 * n + 2, stage2)

    def stage3(k):
        for w in weights:
            add(w, unit(w, 1, 4 + k), (w.first, 4 + k), (w.second, k))
        for w in weights:
            third(w, k).start()

    received(s1_sem.at[2], like[6])
    received(s2_sem.at[0], like[6])
    each(0, 2, stage3)
    loaded(4, like[12])
    loaded(5, like[12])
    loaded(6, like[6])
    sent(all_send.at[0], like[24])
    tell(0, 0)
    received(s1_sem.at[3], like[6])
    sent(all_send.at[1], like[12])
    tell(1, 1)
    received(s2_sem.at[1], like[6])

    def update(k):
        for w in weights:
            third(w, k).wait()
            pl.semaphore_signal(third_free.at[w.i], inc=1, device_id={"dp": w.to[2]}, device_id_type=MESH)
            at = (k, *w.own())

            def body(rows, w=w, at=at):
                g = total(w, at, rows, (w.first, 6 + k), (w.second, 2 + k), (w.third, k)).astype(BF16).astype(F32)
                new, m, v = adamw(w.old[k, rows, :].astype(F32), w.m[k, rows, :], w.v[k, rows, :], g)
                w.m[k, rows, :] = m
                w.v[k, rows, :] = v
                w.all[(*at, core, rows, EVERY)] = new

            slabs(0, w.rows, body)

        for w in weights:
            pl.semaphore_wait(third_free.at[w.i], 1)
            gather3(w, k).start()

    each(0, 2, update)

    def own21(k):
        for w in weights:
            gather2(w, k).start()
        for w in weights:
            gather1(w, k, 0).start()

    told(1)
    told(0)
    each(0, 2, own21)

    pl.semaphore_signal(read_sem, inc=1, device_id={"dp": pair}, device_id_type=MESH)
    pl.semaphore_wait(read_sem, 1)

    def own0(k):
        for w in weights:
            gather0(w, 1, k).start()

    each(0, 2, own0)

    def back3(k):
        for w in weights:
            gather2(w, 2 + k).start()
        for w in weights:
            gather1(w, 2 + k, 1).start()
            gather0(w, 1, 2 + k).start()

    received(a3_sem, like[6])
    each(0, 2, back3)

    def back2(k):
        for w in weights:
            gather0(w, 1, k).start()

    received(a2_sem.at[0], like[6])
    for w in weights:
        gather1(w, 4, 2).start()
    for w in weights:
        gather1(w, 5, 3, 0, w.rows - w.part).start()
    for w in weights:
        gather1(w, 5, 4, w.rows - w.part, w.part).start()
    each(4, 6, back2)
    received(a2_sem.at[1], like[6])
    for w in weights:
        keep_late(w).start()
    each(6, 8, back2)

    def back1(k):
        for w in weights:
            gather0(w, 0, k).start()

    for n in (0, 1):
        received(a1_sem.at[n], like[6])
        each(2 * n, 2 * n + 2, back1)
    for w in weights:
        received(last_sem.at[w.i, 0], w.third.at[0])
        keep_mid(w, 0, 0, w.rows).start()
    for w in weights:
        received(last_sem.at[w.i, 1], w.third.at[0, pl.ds(0, w.rows - w.part)])
        keep_mid(w, 1, 0, w.rows - w.part).start()
    for w in weights:
        received(last_sem.at[w.i, 2], w.third.at[0, pl.ds(0, w.part)])
        keep_mid(w, 1, w.rows - w.part, w.part).start()

    loaded(0, like[6])
    for n, units in ((2, 6), (3, 12), (4, 24), (5, 12)):
        sent(all_send.at[n], like[units])
    received(own_sem, like[24])
    received(a0_sem, like[12])
    for w in weights:
        sent(send_sem.at[w.i, 1], like[6])
    loaded(1, like[6])


def blocks_of(i):
    me = lax.axis_index("dp")
    return Weight(ORDERS[i], [(me // s) % 2 for s in STRIDES], me % 2)


def run(copies):
    for copy in copies:
        copy.start()
    for copy in copies:
        copy.wait()


def put(*refs):
    half = len(refs) // 2
    ins, outs, sem = refs[:half], refs[half:-1], refs[-1]
    copies = []
    for i in range(3):
        w = blocks_of(i)
        here, every = w.own(), EVERY
        coordinates = [here[axis] for axis in w.order]
        for n, at in enumerate((
            (every, *w.place(coordinates[0], every, every)),
            (every, *w.place(1 - coordinates[0], coordinates[1], every)),
            (every, *w.block(0, 0, 1), w.core),
        )):
            copies.append(pltpu.make_async_copy(ins[i].at[at], outs[i].at[at], sem.at[i, n]))
    for j in range(3, half):
        for k in range(LAYERS):
            copies.append(pltpu.make_async_copy(ins[j].at[k], outs[j].at[k], sem.at[j, k]))
    run(copies)


def patch_mid(*refs):
    mids, outs, sem = refs[3:6], refs[6:9], refs[-1]
    copies = []
    for i in range(3):
        w = blocks_of(i)
        copies.append(pltpu.make_async_copy(mids[i], outs[i].at[(EVERY, *w.block(0, 0, 1), 1 - w.core)], sem.at[i]))
    run(copies)


def patch0(*refs):
    rest = 9 - EARLY
    lates, vs, outs, v_outs, sem = refs[3:6], refs[6 : 6 + rest], refs[6 + rest : 9 + rest], refs[9 + rest : -1], refs[-1]
    copies = []
    for i in range(3):
        w = blocks_of(i)
        copies.append(pltpu.make_async_copy(lates[i], outs[i].at[(EVERY, *w.far(), w.core)], sem.at[i, 0]))
    for i in range(rest):
        copies.append(pltpu.make_async_copy(vs[i], v_outs[i], sem.at[i, 1]))
    run(copies)


def patch1(*refs):
    theirs, outs, sem = refs[3:6], refs[6:9], refs[-1]
    copies = []
    for i in range(3):
        w = blocks_of(i)
        copies.append(pltpu.make_async_copy(theirs[i], outs[i].at[(EVERY, *w.far(), 1 - w.core)], sem.at[i]))
    run(copies)


def local(kernel_, outs, hbm, vmem, sems, cost=None):
    return list(
        pl.pallas_call(
            kernel_,
            out_shape=[jax.ShapeDtypeStruct(o.shape, o.dtype) for o in outs],
            in_specs=[pl.BlockSpec(memory_space=pl.ANY)] * len(hbm) + [pl.BlockSpec(memory_space=pltpu.VMEM)] * len(vmem),
            out_specs=[pl.BlockSpec(memory_space=pl.ANY)] * len(outs),
            input_output_aliases={j: j for j in range(len(hbm))},
            scratch_shapes=[pltpu.SemaphoreType.DMA(sems)],
            compiler_params=pltpu.CompilerParams(vmem_limit_bytes=GRANT),
            cost_estimate=cost,
        )(*hbm, *(pltpu.with_memory_space_constraint(o, pltpu.VMEM) for o in vmem))
    )


def solution(mesh):
    def whole_step(*arrays):
        shapes = [a.shape[1:] for a in arrays[6:9]]

        def cut(a, i):
            return a.reshape(*GRID, *shapes[i])

        operands = [cut(a, n % 3) for n, a in enumerate(arrays[:6])] + list(arrays[6:])
        blocks = [(n, rows, columns) for n in (8, 4, 2, LAYERS) for rows, columns in shapes]
        outs = pl.pallas_call(
            kernel,
            out_shape=[pltpu.VMEM((*GRID, *s), BF16) for s in shapes] + [pltpu.VMEM((LAYERS, *s), F32) for s in shapes] * 2 + [jax.ShapeDtypeStruct((LAYERS, *s), BF16) for s in shapes] * 2,
            in_specs=[pl.BlockSpec(memory_space=pl.ANY)] * 12,
            out_specs=[pl.BlockSpec(memory_space=pltpu.VMEM)] * 9 + [pl.BlockSpec(memory_space=pl.ANY)] * 6,
            scratch_shapes=[
                *(pltpu.VMEM(s, BF16) for s in blocks),
                *(pltpu.SemaphoreType.DMA(n) for n in ((8,), (3, 5), (), (4,), (2,), (3, 2), (), (2,), (2,), (3, 3), (), (), (6,), (3, 2), (3, 2))),
                *(pltpu.SemaphoreType.REGULAR(n) for n in ((2,), (3,), ())),
            ],
            compiler_params=pltpu.CompilerParams(collective_id=0, has_side_effects=True, vmem_limit_bytes=GRANT),
            name="step",
        )(*operands)

        def axis(i):
            return lax.ppermute(outs[9 + i], "dp", [(d, d ^ STRIDES[ORDERS[i][0]]) for d in range(16)])

        def over(o):
            return lax.ppermute(o, "dp", [(d, d ^ 1) for d in range(16)])

        late = [axis(i) for i in range(3)]
        mids = [over(o) for o in outs[12:]]
        cost = pl.CostEstimate(flops=PUT_FLOPS, bytes_accessed=2 * 32_000_000, transcendentals=0)
        done = local(put, outs[:EARLY], [], outs[:EARLY], (EARLY, 3), cost)
        for i in range(3):
            late[i], done[3 + i] = lax.optimization_barrier((late[i], done[3 + i]))
        theirs = [over(late[i]) for i in range(2)]
        some = local(patch_mid, done[:3], done[:3], mids, (3,))
        late[2], some[0] = lax.optimization_barrier((late[2], some[0]))
        theirs.append(over(late[2]))
        some = local(patch0, some + list(outs[EARLY:9]), some, [*late, *outs[EARLY:9]], (3, 2))
        weights = local(patch1, done[:3], some[:3], theirs, (3,))
        done = [*weights, *done[3:], *some[3:]]
        whole = [o.reshape(a.shape) for o, a in zip(done[:3], arrays[3:6], strict=True)]
        return (*whole, *done[3:])

    all_of, part = P(None, None, None), P(None, "dp", None)
    return jax.shard_map(
        whole_step,
        mesh=mesh,
        in_specs=(P(("rep", "dp"), None, None, None),) * 3 + (all_of,) * 3 + (part,) * 6,
        out_specs=(P("rep", None, None),) * 3 + (P("rep", "dp", None),) * 6,
        check_vma=False,
    )
```
